128 devices in a mesh: rows: 16 (over z_lo, y, core), width: 8 (over z_hi, x).
Axes of the slice: x: 4, y: 4, z: 4 (z_hi: 2, z_lo: 2; z = z_hi * 2 + z_lo), core: 2. Of those that a mesh axis runs over, the one named last changes fastest.
Arguments:
- one_query: float32 [7168, 7168], P('rows', 'width'), may hold values from -0.09375 to 0.09375
- other_query: float32 [7168, 7168], P('rows', 'width'), may hold values from -0.0625 to 0.0625
- one_key: float32 [7168, 1024], P('rows', 'width'), may hold values from -0.09375 to 0.09375
- other_key: float32 [7168, 1024], P('rows', 'width'), may hold values from -0.0625 to 0.0625
- one_value: float32 [7168, 1024], P('rows', 'width'), may hold values from -0.09375 to 0.09375
- other_value: float32 [7168, 1024], P('rows', 'width'), may hold values from -0.0625 to 0.0625
- mix_share: float32 [7168], P('rows'), may hold values from 0.2 to 0.8
- norm_train: float32 [7168], P(('rows', 'width')), may hold values from 0.25 to 1.75
- norm_step: float32 [7168], P(('rows', 'width')), may hold values from -0.3 to 0.3
Outputs:
- final_query: bfloat16 [7168, 7168], P(None, 'width')
- final_key: bfloat16 [7168, 1024], P(None, 'width')
- final_value: bfloat16 [7168, 1024], P(None, 'width')
- column_query: float32 [7168], P('width')
- column_key: float32 [1024], P('width')
- column_value: float32 [1024], P('width')
- serve_norm: bfloat16 [7168], replicated
The draws below stay inside these ranges and needn't reach their ends.
All inputs are finite; a program needn't handle non-finite values.
Results may differ from the reference program's by a relative error of at most 0.001.
Values may be sent and summed in bfloat16 or wider, within the bound.
A program may use at most 128 MiB of HBM per device.

```python
import jax
import jax.numpy as jnp
from jax import lax

D_MODEL = 7168
Q_DIM = 7168
KV_DIM = 1024


def spiked(result, rng, source, target, shards_of, factor):
    owner, partner = [(jnp.arange(result.shape[position]) // (result.shape[position] // shards_of)).reshape([-1 if axis == position else 1 for axis in range(result.ndim)]) for position in (source, target)]
    chosen = jax.random.permutation(rng, shards_of)[partner]
    strong = (owner == chosen) | (owner == (partner + shards_of // 2) % shards_of)
    return jnp.where(strong, factor * result, result)


def block_levels(stream_key, shape, shards, smallest, top_value):
    def one(position, shards_of):
        heights = jax.random.uniform(jax.random.fold_in(jax.random.fold_in(stream_key, 6), position), (shards_of,), jnp.float32, smallest / len(shards), top_value / len(shards))
        return jnp.repeat(jnp.exp(heights), shape[position] // shards_of).reshape((-1,) + (1,) * (len(shape) - position - 1))

    loudness = one(*shards[0])
    for cut in shards[1:]:
        loudness = loudness * one(*cut)
    return loudness


def bell_draw(rng, dims, deviation, most, cuts=(), dtype=jnp.bfloat16):
    entries = jax.random.normal(rng, dims, jnp.float32) * deviation
    if len(cuts) > 0:
        entries = block_levels(rng, dims, cuts, -0.22, 0.18) * entries
    return jnp.clip(entries, min=-most, max=most).astype(dtype)


def heavy_noise(key, extent, scale, most, split, heavy, dtype=jnp.bfloat16):
    values = scale * jax.random.normal(key, extent, jnp.float32)
    if split:
        values = values * block_levels(key, extent, split, -0.22, 0.18)
    return jnp.clip(spiked(values, jax.random.fold_in(key, 3), *heavy), -most, most).astype(dtype)


def setup_inputs(seed: int = 0) -> dict:
    seeds = jax.random.split(jax.random.key(seed), 10)
    return {
        "one_query": heavy_noise(seeds[0], (D_MODEL, Q_DIM), D_MODEL ** -0.5, 0.09375, ((0, 16), (1, 8)), (0, 1, 16, 2.0), jnp.float32),
        "other_query": bell_draw(seeds[1], (D_MODEL, Q_DIM), D_MODEL ** -0.5, 0.0625, ((0, 16), (1, 8)), jnp.float32),
        "one_key": heavy_noise(seeds[2], (D_MODEL, KV_DIM), D_MODEL ** -0.5, 0.09375, ((0, 16), (1, 8)), (0, 1, 16, 2.0), jnp.float32),
        "other_key": bell_draw(seeds[3], (D_MODEL, KV_DIM), D_MODEL ** -0.5, 0.0625, ((0, 16), (1, 8)), jnp.float32),
        "one_value": heavy_noise(seeds[4], (D_MODEL, KV_DIM), D_MODEL ** -0.5, 0.09375, ((0, 16), (1, 8)), (0, 1, 16, 2.0), jnp.float32),
        "other_value": bell_draw(seeds[5], (D_MODEL, KV_DIM), D_MODEL ** -0.5, 0.0625, ((0, 16), (1, 8)), jnp.float32),
        "mix_share": jnp.clip(0.2 + 0.6 * jax.random.uniform(seeds[6], (D_MODEL,), jnp.float32) ** block_levels(seeds[6], (D_MODEL,), ((0, 16),), -0.2, 0.2), 0.2, 0.8),
        "norm_train": jnp.clip(1.0 + 0.15 * jax.random.normal(seeds[7], (D_MODEL,), jnp.float32), 0.25, 1.75),
        "norm_step": jnp.clip(jax.random.uniform(seeds[8], (D_MODEL,), jnp.float32, -0.3, 0.3) * block_levels(seeds[8], (D_MODEL,), ((0, 128),), -0.4, 0.0), -0.3, 0.3),
    }


def reference(one_query, other_query, one_key, other_key, one_value, other_value, mix_share, norm_train, norm_step):
    result_query = mix_share[:, None] * one_query + (1.0 - mix_share[:, None]) * other_query
    result_key = mix_share[:, None] * one_key + (1.0 - mix_share[:, None]) * other_key
    result_value = mix_share[:, None] * one_value + (1.0 - mix_share[:, None]) * other_value
    column_query = jnp.sqrt(lax.optimization_barrier(jnp.sum(result_query * result_query, axis=0)))
    final_query = (result_query / column_query).astype(jnp.bfloat16)
    column_key = jnp.sqrt(lax.optimization_barrier(jnp.sum(result_key * result_key, axis=0)))
    final_key = (result_key / column_key).astype(jnp.bfloat16)
    column_value = jnp.sqrt(lax.optimization_barrier(jnp.sum(result_value * result_value, axis=0)))
    final_value = (result_value / column_value).astype(jnp.bfloat16)
    serve_norm = (norm_train + norm_step).astype(jnp.bfloat16)
    return (final_query, final_key, final_value, column_query, column_key, column_value, serve_norm)
```

```python
import jax
import jax.numpy as jnp
from jax import lax
from jax.experimental import pallas as pl
from jax.experimental.pallas import tpu as pltpu
from jax.sharding import PartitionSpec as P

MESH = pl.DeviceIdType.MESH
LANES = 128
CIRCLE = 4
UP, DOWN, ACROSS = 0, 1, 2


def split_groups(count):
    first = [g for g in range(count) if g % 2 == 0]
    return first, [g for g in range(count) if g % 2]


def plan(count, cross_first):
    free = [0.0, 0.0, 0.0]
    flying = []

    def send(now, item):
        link, _, hop, _ = item
        half = hop == 2 if link != ACROSS else hop >= 3
        free[link] = max(free[link], now) + (0.5 if half else 1.0)
        flying.append((free[link], len(flying), item))

    for g in range(count):
        send(0.0, (UP, 0, 1, g))
        send(0.0, (DOWN, 0, 1, g))
        send(0.0, (ACROSS, 0, 0, g))
    order = []
    while flying:
        flying.sort()
        now, _, item = flying.pop(0)
        now += 0.5
        steps = followers(item, cross_first)
        order.append((item, steps))
        for step in steps:
            send(now, step)
    return order


def followers(item, cross_first):
    link, far, hop, g = item
    if link == ACROSS:
        return [(UP, 1, 1, g), (DOWN, 1, 1, g)] if g in cross_first else []
    steps = [(link, far, 2, g)] if hop == 1 else []
    if g not in cross_first:
        steps.append((ACROSS, 0, 1 + link if hop == 1 else 3 + link, g))
    return steps


def kernel(
    n_rows,
    n_width,
    share_in,
    norm_train,
    norm_step,
    one_query,
    other_query,
    one_key,
    other_key,
    one_value,
    other_value,
    *refs,
):
    blocks = refs[: 2 + one_query.shape[1] // one_key.shape[1]]
    col_query, col_key, col_value, norm_all, first, second, share = refs[len(blocks) :][:7]
    line, train, step, part, in_sem, small_sem = refs[len(blocks) + 7 :][:6]
    norm_send, norm_recv, slab_send, slab_recv, sum_send, sum_recv = refs[len(blocks) + 13 :][:6]
    ring_send, ring_recv, pair_send, pair_recv, twin_send, twin_recv = refs[len(blocks) + 19 :]
    me = lax.axis_index("rows")
    lane = lax.axis_index("width")
    depth, wide = one_key.shape
    groups = [
        (one_key, other_key, blocks[0], col_key, 0),
        (one_value, other_value, blocks[1], col_value, 0),
    ] + [
        (one_query, other_query, blocks[2 + j], col_query, j * wide)
        for j in range(one_query.shape[1] // wide)
    ]
    count = len(groups)
    tile = 64 if depth % 64 == 0 else 16
    half = depth // 2

    small = []
    for i, (src, dst) in enumerate(((share_in, line), (norm_train, train), (norm_step, step))):
        small.append(pltpu.make_async_copy(src, dst, small_sem.at[i]))
        small[-1].start()
    loads = []
    for g, (one, other, _, _, at) in enumerate(groups):
        a = pltpu.make_async_copy(one.at[:, pl.ds(at, wide)], first.at[g], in_sem.at[0, g])
        b = pltpu.make_async_copy(other.at[:, pl.ds(at, wide)], second.at[g], in_sem.at[1, g])
        loads.append((a, b))
        a.start()
        b.start()

    barrier = pltpu.get_barrier_semaphore()
    for d in range(1, n_rows):
        pl.semaphore_signal(
            barrier, inc=1, device_id={"rows": lax.rem(me + d, n_rows)}, device_id_type=MESH
        )
    for d in range(1, n_width):
        pl.semaphore_signal(
            barrier, inc=1, device_id={"width": lax.rem(lane + d, n_width)}, device_id_type=MESH
        )

    for copy in small:
        copy.wait()
    norm_all[me, lane] = (train[...] + step[...]).reshape(1, -1)
    for at in range(0, depth, LANES):
        size = min(LANES, depth - at)
        piece = line[pl.ds(at, size)].reshape(1, size)
        share[pl.ds(at, size), :] = jnp.broadcast_to(piece, (LANES, size)).T

    for g in range(count):
        for load in loads[g]:
            load.wait()

        def mix(i, acc):
            rows = pl.ds(pl.multiple_of(i * tile, tile), tile)
            s = share[rows, :]
            s = jnp.concatenate([s] * (wide // LANES), axis=1)
            r = s * first[g, rows, :] + (1.0 - s) * second[g, rows, :]
            first[g, rows, :] = r
            return acc + jnp.sum((r * r).reshape(tile // 8, 8, wide), axis=0)

        acc = lax.fori_loop(0, depth // tile, mix, jnp.zeros((8, wide), jnp.float32))
        part[me, pl.ds(g, 1), :] = jnp.sum(acc, axis=0, keepdims=True)

    pl.semaphore_wait(barrier, n_rows + n_width - 2)

    sums = []
    for d in range(1, n_rows):
        copy = pltpu.make_async_remote_copy(
            src_ref=part.at[me],
            dst_ref=part.at[me],
            send_sem=sum_send.at[d],
            recv_sem=sum_recv.at[d],
            device_id={"rows": lax.rem(me + d, n_rows)},
            device_id_type=MESH,
        )
        copy.start()
        sums.append(copy)
    norm_copies = []
    for d in range(1, n_width):
        copy = pltpu.make_async_remote_copy(
            src_ref=norm_all.at[me, lane],
            dst_ref=norm_all.at[me, lane],
            send_sem=norm_send.at[d],
            recv_sem=norm_recv.at[d],
            device_id={"width": lax.rem(lane + d, n_width)},
            device_id_type=MESH,
        )
        copy.start()
        norm_copies.append(copy)

    core = me % 2
    place = (me // 2) % CIRCLE
    side = me // (2 * CIRCLE)

    def device(sides, steps):
        return ((side + sides) % 2 * CIRCLE + (place + steps + CIRCLE) % CIRCLE) * 2 + core

    twin = me + 1 - 2 * core
    target = {UP: device(0, 1), DOWN: device(0, -1), ACROSS: device(1, 0)}
    waits = []

    def whole(owner):
        return pl.ds(pl.multiple_of(owner * depth, half), depth)

    def part_of(owner, way):
        return pl.ds(pl.multiple_of(owner * depth + way * half, half), half)

    def rows_of(item, sender):
        link, far, hop, _ = item
        if link == ACROSS:
            side_of = 0 if sender else 1
            if hop >= 3:
                return part_of(device(side_of, 2), hop - 3)
            return whole(device(side_of, (0, -1, 1)[hop]))
        away = hop - 1 if sender else hop
        owner = device(far, -away if link == UP else away)
        return whole(owner) if hop == 1 else part_of(owner, link)

    def remote(item, sender):
        link, far, hop, g = item
        ref = blocks[g].at[rows_of(item, sender), :]
        if link == ACROSS:
            sems = pair_send.at[hop, g], pair_recv.at[hop, g]
        else:
            sems = ring_send.at[link, far, hop - 1, g], ring_recv.at[link, far, hop - 1, g]
        return pltpu.make_async_remote_copy(
            src_ref=ref,
            dst_ref=ref,
            send_sem=sems[0],
            recv_sem=sems[1],
            device_id={"rows": target[link]},
            device_id_type=MESH,
        )

    def send(item):
        copy = remote(item, True)
        copy.start()
        waits.append(copy)

    twins = []

    def share_with_twin(g, rows, slot):
        ref = blocks[g].at[rows, :]
        copy = pltpu.make_async_remote_copy(
            src_ref=ref,
            dst_ref=ref,
            send_sem=twin_send.at[slot, g],
            recv_sem=twin_recv.at[slot, g],
            device_id={"rows": twin},
            device_id_type=MESH,
        )
        copy.start()
        twins.append(copy)

    for copy in sums:
        copy.wait_recv()
    total = part[0]
    for p in range(1, n_rows):
        total = total + part[p]
    scale = jnp.sqrt(total)
    inverse = 1.0 / scale

    def release(g):
        send((ACROSS, 0, 0, g))
        send((UP, 0, 1, g))
        send((DOWN, 0, 1, g))
        share_with_twin(g, whole(me), 0)

    for g, (_, _, out, col, at) in enumerate(groups):
        col[pl.ds(at, wide)] = scale[g : g + 1, :].reshape(wide)
        by = inverse[g : g + 1, :]

        def narrow(i, carry):
            rows = pl.ds(pl.multiple_of(i * tile, tile), tile)
            here = pl.ds(pl.multiple_of(me * depth + i * tile, tile), tile)
            out[here, :] = (first[g, rows, :] * by).astype(out.dtype)
            return carry

        lax.fori_loop(0, depth // tile, narrow, 0)
        if g:
            release(g - 1)
    release(count - 1)

    for copy in norm_copies:
        copy.wait_recv()
    slab_copies = []
    for d in range(1, n_rows):
        copy = pltpu.make_async_remote_copy(
            src_ref=norm_all.at[me],
            dst_ref=norm_all.at[me],
            send_sem=slab_send.at[d],
            recv_sem=slab_recv.at[d],
            device_id={"rows": lax.rem(me + d, n_rows)},
            device_id_type=MESH,
        )
        copy.start()
        slab_copies.append(copy)

    cross_first, _ = split_groups(count)
    slots = [1] * count
    for item, steps in plan(count, cross_first):
        g = item[3]
        remote(item, False).wait_recv()
        for step_on in steps:
            send(step_on)
        share_with_twin(g, rows_of(item, False), slots[g])
        slots[g] += 1

    for copy in waits:
        copy.wait_send()
    for copy in twins:
        copy.wait()
    for copy in norm_copies + sums:
        copy.wait_send()
    for copy in slab_copies:
        copy.wait()


def store(*refs):
    outs, sem = refs[-8:-1], refs[-1]
    blocks, small = refs[:-12], refs[-12:-8]
    wide = blocks[0].shape[1]
    pairs = [(blocks[0], outs[1]), (blocks[1], outs[2])] + list(zip(small, outs[3:]))
    for j, block in enumerate(blocks[2:]):
        pairs.append((block, outs[0].at[:, pl.ds(j * wide, wide)]))
    copies = [pltpu.make_async_copy(src, dst, sem.at[i]) for i, (src, dst) in enumerate(pairs)]
    for copy in copies:
        copy.start()
    for copy in copies:
        copy.wait()


def solution(mesh):
    n_rows, n_width = mesh.shape["rows"], mesh.shape["width"]

    def shards(
        one_query,
        other_query,
        one_key,
        other_key,
        one_value,
        other_value,
        mix_share,
        norm_train,
        norm_step,
    ):
        depth, wide = one_key.shape
        wide_query = one_query.shape[1]
        count = 2 + wide_query // wide
        piece = norm_train.shape[0]
        total = depth * n_rows
        hbm = pl.BlockSpec(memory_space=pltpu.HBM)
        vmem = pl.BlockSpec(memory_space=pltpu.VMEM)
        dma = pltpu.SemaphoreType.DMA
        out_shape = (pltpu.VMEM((total, wide), jnp.bfloat16),) * count + (
            pltpu.VMEM((wide_query,), jnp.float32),
            pltpu.VMEM((wide,), jnp.float32),
            pltpu.VMEM((wide,), jnp.float32),
            pltpu.VMEM((n_rows, n_width, 1, piece), jnp.float32),
        )
        gathered = pl.pallas_call(
            lambda *refs: kernel(n_rows, n_width, *refs),
            out_shape=out_shape,
            in_specs=[hbm] * 9,
            out_specs=[vmem] * (count + 4),
            scratch_shapes=[
                pltpu.VMEM((count, depth, wide), jnp.float32),
                pltpu.VMEM((count, depth, wide), jnp.float32),
                pltpu.VMEM((depth, LANES), jnp.float32),
                pltpu.VMEM((depth,), jnp.float32),
                pltpu.VMEM((piece,), jnp.float32),
                pltpu.VMEM((piece,), jnp.float32),
                pltpu.VMEM((n_rows, count, wide), jnp.float32),
                dma((2, count)),
                dma((3,)),
                dma((n_width,)),
                dma((n_width,)),
                dma((n_rows,)),
                dma((n_rows,)),
                dma((n_rows,)),
                dma((n_rows,)),
                dma((2, 2, 2, count)),
                dma((2, 2, 2, count)),
                dma((5, count)),
                dma((5, count)),
                dma((10, count)),
                dma((10, count)),
            ],
            compiler_params=pltpu.CompilerParams(
                collective_id=0, has_side_effects=True, vmem_limit_bytes=44 * 1024 * 1024
            ),
        )(mix_share, norm_train, norm_step, one_query, other_query, one_key, other_key, one_value, other_value)
        final_query, final_key, final_value, col_query, col_key, col_value, norm_all = pl.pallas_call(
            store,
            out_shape=(
                jax.ShapeDtypeStruct((total, wide_query), jnp.bfloat16),
                jax.ShapeDtypeStruct((total, wide), jnp.bfloat16),
                jax.ShapeDtypeStruct((total, wide), jnp.bfloat16),
            )
            + tuple(jax.ShapeDtypeStruct(o.shape, o.dtype) for o in out_shape[count:]),
            in_specs=[vmem] * (count + 4),
            out_specs=[hbm] * 7,
            scratch_shapes=[dma((count + 4,))],
            compiler_params=pltpu.CompilerParams(vmem_limit_bytes=1024 * 1024),
        )(*gathered)
        serve_norm = norm_all[..., 0, :].astype(jnp.bfloat16).reshape(-1)
        return (
            final_query,
            final_key,
            final_value,
            col_query,
            col_key,
            col_value,
            serve_norm,
        )

    wide_spec = P("rows", "width")
    in_specs = (wide_spec,) * 6 + (P("rows"), P(("rows", "width")), P(("rows", "width")))
    out_specs = (P(None, "width"),) * 3 + (P("width"),) * 3 + (P(),)
    return jax.shard_map(shards, mesh=mesh, in_specs=in_specs, out_specs=out_specs, check_vma=False)
```

```python
import jax
import jax.numpy as jnp
from jax import lax
from jax.experimental import pallas as pl
from jax.experimental.pallas import tpu as pltpu
from jax.sharding import PartitionSpec as P

MESH = pl.DeviceIdType.MESH
LANES = 128
CIRCLE = 4
UP, DOWN, ACROSS = 0, 1, 2


def split_groups(count):
    first = [g for g in range(count) if g % 2 == 0]
    return first, [g for g in range(count) if g % 2]


def plan(count, cross_first):
    free = [0.0, 0.0, 0.0]
    flying = []

    def send(now, item):
        link = item[0]
        free[link] = max(free[link], now) + (1.0 if is_whole(item) else 0.5)
        flying.append((free[link], len(flying), item))

    for g in range(count):
        send(0.0, (UP, 0, 1, g))
        send(0.0, (DOWN, 0, 1, g))
        send(0.0, (ACROSS, 0, 0, g))
    order = []
    while flying:
        flying.sort()
        now, _, item = flying.pop(0)
        now += 0.5
        steps = followers(item, cross_first)
        order.append((item, steps))
        for step in steps:
            send(now, step)
    return order


def is_whole(item):
    link, _, hop, _ = item
    return hop < 3 if link == ACROSS else hop == 1


def followers(item, cross_first):
    link, far, hop, g = item
    if link == ACROSS:
        return [(UP, 1, 1, g), (DOWN, 1, 1, g)] if g in cross_first else []
    steps = [(link, far, 2, g)] if hop == 1 else []
    if g not in cross_first:
        steps.append((ACROSS, 0, 1 + link if hop == 1 else 3 + link, g))
    return steps


def kernel(
    n_rows,
    n_width,
    share_in,
    norm_train,
    norm_step,
    one_query,
    other_query,
    one_key,
    other_key,
    one_value,
    other_value,
    *refs,
):
    blocks = refs[: 2 + one_query.shape[1] // one_key.shape[1]]
    col_query, col_key, col_value, norm_all, mixed, share = refs[len(blocks) :][:6]
    line, train, step, part, in_sem, small_sem = refs[len(blocks) + 6 :][:6]
    norm_sem, slab_sem, sum_sem, send_sem = refs[len(blocks) + 12 :][:4]
    ring_recv, pair_recv, twin_sem = refs[len(blocks) + 16 :]
    me = lax.axis_index("rows")
    lane = lax.axis_index("width")
    depth, wide = one_key.shape
    groups = [
        (one_key, other_key, blocks[0], col_key, 0),
        (one_value, other_value, blocks[1], col_value, 0),
    ] + [
        (one_query, other_query, blocks[2 + j], col_query, j * wide)
        for j in range(one_query.shape[1] // wide)
    ]
    count = len(groups)
    tile = 64 if depth % 64 == 0 else 16
    half = depth // 2

    def drain(ref, sem):
        pltpu.make_async_copy(ref, ref, sem).wait()

    small = []
    for i, (src, dst) in enumerate(((share_in, line), (norm_train, train), (norm_step, step))):
        small.append(pltpu.make_async_copy(src, dst, small_sem.at[i]))
        small[-1].start()
    for g, (one, other, _, _, at) in enumerate(groups):
        a = pltpu.make_async_copy(one.at[:, pl.ds(at, wide)], mixed.at[g, 0], in_sem.at[g])
        b = pltpu.make_async_copy(other.at[:, pl.ds(at, wide)], mixed.at[g, 1], in_sem.at[g])
        a.start()
        b.start()

    barrier = pltpu.get_barrier_semaphore()
    for d in range(1, n_rows):
        pl.semaphore_signal(
            barrier, inc=1, device_id={"rows": lax.rem(me + d, n_rows)}, device_id_type=MESH
        )
    for d in range(1, n_width):
        pl.semaphore_signal(
            barrier, inc=1, device_id={"width": lax.rem(lane + d, n_width)}, device_id_type=MESH
        )

    for copy in small:
        copy.wait()
    norm_all[me, lane] = (train[...] + step[...]).reshape(1, -1)
    for at in range(0, depth, LANES):
        size = min(LANES, depth - at)
        piece = line[pl.ds(at, size)].reshape(1, size)
        share[pl.ds(at, size), :] = jnp.broadcast_to(piece, (LANES, size)).T

    for g in range(count):
        drain(mixed.at[g], in_sem.at[g])

        def mix(i, acc):
            rows = pl.ds(pl.multiple_of(i * tile, tile), tile)
            s = share[rows, :]
            s = jnp.concatenate([s] * (wide // LANES), axis=1)
            r = s * mixed[g, 0, rows, :] + (1.0 - s) * mixed[g, 1, rows, :]
            mixed[g, 0, rows, :] = r
            return acc + jnp.sum((r * r).reshape(tile // 8, 8, wide), axis=0)

        acc = lax.fori_loop(0, depth // tile, mix, jnp.zeros((8, wide), jnp.float32))
        part[me, pl.ds(g, 1), :] = jnp.sum(acc, axis=0, keepdims=True)

    pl.semaphore_wait(barrier, n_rows + n_width - 2)

    def to_others(ref, sems, axis, mine, size):
        for d in range(1, size):
            pltpu.make_async_remote_copy(
                src_ref=ref,
                dst_ref=ref,
                send_sem=sems.at[0],
                recv_sem=sems.at[1],
                device_id={axis: lax.rem(mine + d, size)},
                device_id_type=MESH,
            ).start()

    to_others(part.at[me], sum_sem, "rows", me, n_rows)
    to_others(norm_all.at[me, lane], norm_sem, "width", lane, n_width)

    cross_first, _ = split_groups(count)

    def bucket(g):
        return 2 * g // (count + 1)

    core = me % 2
    place = (me // 2) % CIRCLE
    side = me // (2 * CIRCLE)

    def device(sides, steps):
        return ((side + sides) % 2 * CIRCLE + (place + steps + CIRCLE) % CIRCLE) * 2 + core

    twin = me + 1 - 2 * core
    target = {UP: device(0, 1), DOWN: device(0, -1), ACROSS: device(1, 0)}
    def whole(owner):
        return pl.ds(pl.multiple_of(owner * depth, half), depth)

    def part_of(owner, way):
        return pl.ds(pl.multiple_of(owner * depth + way * half, half), half)

    def rows_of(item, sender):
        link, far, hop, _ = item
        if link == ACROSS:
            side_of = 0 if sender else 1
            if hop >= 3:
                return part_of(device(side_of, 2), hop - 3)
            return whole(device(side_of, (0, -1, 1)[hop]))
        away = hop - 1 if sender else hop
        owner = device(far, -away if link == UP else away)
        return whole(owner) if hop == 1 else part_of(owner, link)

    def remote(item, sender):
        link, far, hop, g = item
        ref = blocks[g].at[rows_of(item, sender), :]
        if link == ACROSS:
            arrived = pair_recv.at[hop, g]
        else:
            arrived = ring_recv.at[link, far, hop - 1, g]
        return pltpu.make_async_remote_copy(
            src_ref=ref,
            dst_ref=ref,
            send_sem=send_sem.at[link, bucket(g)],
            recv_sem=arrived,
            device_id={"rows": target[link]},
            device_id_type=MESH,
        )

    sent = {}

    def send(item):
        remote(item, True).start()
        link, _, hop, g = item
        key = link, bucket(g)
        sent[key] = sent.get(key, 0) + (depth if is_whole(item) else half)

    def share_with_twin(g, rows):
        ref = blocks[g].at[rows, :]
        pltpu.make_async_remote_copy(
            src_ref=ref,
            dst_ref=ref,
            send_sem=twin_sem.at[0, g],
            recv_sem=twin_sem.at[1, g],
            device_id={"rows": twin},
            device_id_type=MESH,
        ).start()

    others = part.at[pl.ds(0, n_rows - 1)]
    drain(others, sum_sem.at[1])
    total = part[0]
    for p in range(1, n_rows):
        total = total + part[p]
    scale = jnp.sqrt(total)
    inverse = 1.0 / scale

    def release(g):
        send((ACROSS, 0, 0, g))
        send((UP, 0, 1, g))
        send((DOWN, 0, 1, g))
        share_with_twin(g, whole(me))

    for g, (_, _, out, col, at) in enumerate(groups):
        col[pl.ds(at, wide)] = scale[g : g + 1, :].reshape(wide)
        by = inverse[g : g + 1, :]

        def narrow(i, carry):
            rows = pl.ds(pl.multiple_of(i * tile, tile), tile)
            here = pl.ds(pl.multiple_of(me * depth + i * tile, tile), tile)
            out[here, :] = (mixed[g, 0, rows, :] * by).astype(out.dtype)
            return carry

        lax.fori_loop(0, depth // tile, narrow, 0)
        if g:
            release(g - 1)
    release(count - 1)

    lanes = norm_all.at[0, pl.ds(0, n_width - 1)]
    drain(lanes, norm_sem.at[1])
    to_others(norm_all.at[me], slab_sem, "rows", me, n_rows)

    for item, steps in plan(count, cross_first):
        g = item[3]
        remote(item, False).wait_recv()
        for step_on in steps:
            send(step_on)
        share_with_twin(g, rows_of(item, False))

    for (link, key), rows in sent.items():
        drain(blocks[0].at[pl.ds(0, rows), :], send_sem.at[link, key])
    for g, block in enumerate(blocks):
        for way in range(2):
            drain(block.at[pl.ds(0, depth * n_rows // 2), :], twin_sem.at[way, g])
    drain(lanes, norm_sem.at[0])
    drain(others, sum_sem.at[0])
    for way in range(2):
        drain(norm_all.at[pl.ds(0, n_rows - 1)], slab_sem.at[way])


def store(*refs):
    outs, sem = refs[-8:-1], refs[-1]
    blocks, small = refs[:-12], refs[-12:-8]
    wide = blocks[0].shape[1]
    pairs = [(blocks[0], outs[1]), (blocks[1], outs[2])] + list(zip(small, outs[3:]))
    for j, block in enumerate(blocks[2:]):
        pairs.append((block, outs[0].at[:, pl.ds(j * wide, wide)]))
    copies = [pltpu.make_async_copy(src, dst, sem.at[i]) for i, (src, dst) in enumerate(pairs)]
    for copy in copies:
        copy.start()
    for copy in copies:
        copy.wait()


def solution(mesh):
    n_rows, n_width = mesh.shape["rows"], mesh.shape["width"]

    def shards(
        one_query,
        other_query,
        one_key,
        other_key,
        one_value,
        other_value,
        mix_share,
        norm_train,
        norm_step,
    ):
        depth, wide = one_key.shape
        wide_query = one_query.shape[1]
        count = 2 + wide_query // wide
        piece = norm_train.shape[0]
        total = depth * n_rows
        hbm = pl.BlockSpec(memory_space=pltpu.HBM)
        vmem = pl.BlockSpec(memory_space=pltpu.VMEM)
        dma = pltpu.SemaphoreType.DMA
        out_shape = (pltpu.VMEM((total, wide), jnp.bfloat16),) * count + (
            pltpu.VMEM((wide_query,), jnp.float32),
            pltpu.VMEM((wide,), jnp.float32),
            pltpu.VMEM((wide,), jnp.float32),
            pltpu.VMEM((n_rows, n_width, 1, piece), jnp.float32),
        )
        gathered = pl.pallas_call(
            lambda *refs: kernel(n_rows, n_width, *refs),
            out_shape=out_shape,
            in_specs=[hbm] * 9,
            out_specs=[vmem] * (count + 4),
            scratch_shapes=[
                pltpu.VMEM((count, 2, depth, wide), jnp.float32),
                pltpu.VMEM((depth, LANES), jnp.float32),
                pltpu.VMEM((depth,), jnp.float32),
                pltpu.VMEM((piece,), jnp.float32),
                pltpu.VMEM((piece,), jnp.float32),
                pltpu.VMEM((n_rows, count, wide), jnp.float32),
                dma((count,)),
                dma((3,)),
                dma((2,)),
                dma((2,)),
                dma((2,)),
                dma((3, 2)),
                dma((2, 2, 2, count)),
                dma((5, count)),
                dma((2, count)),
            ],
            compiler_params=pltpu.CompilerParams(
                collective_id=0, has_side_effects=True, vmem_limit_bytes=44 * 1024 * 1024
            ),
        )(mix_share, norm_train, norm_step, one_query, other_query, one_key, other_key, one_value, other_value)
        final_query, final_key, final_value, col_query, col_key, col_value, norm_all = pl.pallas_call(
            store,
            out_shape=(
                jax.ShapeDtypeStruct((total, wide_query), jnp.bfloat16),
                jax.ShapeDtypeStruct((total, wide), jnp.bfloat16),
                jax.ShapeDtypeStruct((total, wide), jnp.bfloat16),
            )
            + tuple(jax.ShapeDtypeStruct(o.shape, o.dtype) for o in out_shape[count:]),
            in_specs=[vmem] * (count + 4),
            out_specs=[hbm] * 7,
            scratch_shapes=[dma((count + 4,))],
            compiler_params=pltpu.CompilerParams(vmem_limit_bytes=1024 * 1024),
        )(*gathered)
        serve_norm = norm_all[..., 0, :].astype(jnp.bfloat16).reshape(-1)
        return (
            final_query,
            final_key,
            final_value,
            col_query,
            col_key,
            col_value,
            serve_norm,
        )

    wide_spec = P("rows", "width")
    in_specs = (wide_spec,) * 6 + (P("rows"), P(("rows", "width")), P(("rows", "width")))
    out_specs = (P(None, "width"),) * 3 + (P("width"),) * 3 + (P(),)
    return jax.shard_map(shards, mesh=mesh, in_specs=in_specs, out_specs=out_specs, check_vma=False)
```

```python
import jax
import jax.numpy as jnp
from jax import lax
from jax.experimental import pallas as pl
from jax.experimental.pallas import tpu as pltpu
from jax.sharding import PartitionSpec as P

MESH = pl.DeviceIdType.MESH
LANES = 128
CIRCLE = 4
UP, DOWN, ACROSS = 0, 1, 2


def split_groups(count):
    first = [g for g in range(count) if g % 2 == 0]
    return first, [g for g in range(count) if g % 2]


def plan(count, cross_first):
    free = [0.0, 0.0, 0.0]
    flying = []

    def send(now, item):
        link = item[0]
        free[link] = max(free[link], now) + (1.0 if is_whole(item) else 0.5)
        flying.append((free[link], len(flying), item))

    for g in range(count):
        send(0.0, (UP, 0, 1, g))
        send(0.0, (DOWN, 0, 1, g))
        send(0.0, (ACROSS, 0, 0, g))
    order = []
    while flying:
        flying.sort()
        now, _, item = flying.pop(0)
        now += 0.5
        steps = followers(item, cross_first)
        order.append((item, steps))
        for step in steps:
            send(now, step)
    return order


def is_whole(item):
    link, _, hop, _ = item
    return hop < 3 if link == ACROSS else hop == 1


def followers(item, cross_first):
    link, far, hop, g = item
    if link == ACROSS:
        return [(UP, 1, 1, g), (DOWN, 1, 1, g)] if g in cross_first else []
    steps = [(link, far, 2, g)] if hop == 1 else []
    if g not in cross_first:
        steps.append((ACROSS, 0, 1 + link if hop == 1 else 3 + link, g))
    return steps


def kernel(
    n_rows,
    n_width,
    share_in,
    norm_train,
    norm_step,
    one_query,
    other_query,
    one_key,
    other_key,
    one_value,
    other_value,
    *refs,
):
    blocks = refs[: 2 + one_query.shape[1] // one_key.shape[1]]
    col_query, col_key, col_value, serve, mixed, share = refs[len(blocks) :][:6]
    line, train, step, part, slab, flat, in_sem, small_sem = refs[len(blocks) + 6 :][:8]
    slab_sem, relay_send, relay_recv, sum_sem, send_sem = refs[len(blocks) + 14 :][:5]
    ring_recv, pair_recv, twin_sem = refs[len(blocks) + 19 :]
    me = lax.axis_index("rows")
    lane = lax.axis_index("width")
    depth, wide = one_key.shape
    groups = [
        (one_key, other_key, blocks[0], col_key, 0),
        (one_value, other_value, blocks[1], col_value, 0),
    ] + [
        (one_query, other_query, blocks[2 + j], col_query, j * wide)
        for j in range(one_query.shape[1] // wide)
    ]
    count = len(groups)
    tile = 64 if depth % 64 == 0 else 16
    half = depth // 2

    def drain(ref, sem):
        pltpu.make_async_copy(ref, ref, sem).wait()

    small = []
    for i, (src, dst) in enumerate(((share_in, line), (norm_train, train), (norm_step, step))):
        small.append(pltpu.make_async_copy(src, dst, small_sem.at[i]))
        small[-1].start()
    for g, (one, other, _, _, at) in enumerate(groups):
        a = pltpu.make_async_copy(one.at[:, pl.ds(at, wide)], mixed.at[g, 0], in_sem.at[g])
        b = pltpu.make_async_copy(other.at[:, pl.ds(at, wide)], mixed.at[g, 1], in_sem.at[g])
        a.start()
        b.start()

    barrier = pltpu.get_barrier_semaphore()
    for d in range(1, n_rows):
        pl.semaphore_signal(
            barrier, inc=1, device_id={"rows": lax.rem(me + d, n_rows)}, device_id_type=MESH
        )

    envoy = me == 0

    @pl.when(envoy)
    def _():
        for d in range(1, n_width):
            pl.semaphore_signal(
                barrier, inc=1, device_id={"width": lax.rem(lane + d, n_width)}, device_id_type=MESH
            )

    for copy in small:
        copy.wait()
    piece_size = norm_train.shape[0]
    part[me, pl.ds(count, 1), :] = jnp.zeros((1, wide), jnp.float32)
    part[me, pl.ds(count, 1), pl.ds(0, piece_size)] = (train[...] + step[...]).reshape(1, -1)
    for at in range(0, depth, LANES):
        size = min(LANES, depth - at)
        piece = line[pl.ds(at, size)].reshape(1, size)
        share[pl.ds(at, size), :] = jnp.broadcast_to(piece, (LANES, size)).T

    for g in range(count):
        drain(mixed.at[g], in_sem.at[g])

        def mix(i, acc):
            rows = pl.ds(pl.multiple_of(i * tile, tile), tile)
            s = share[rows, :]
            s = jnp.concatenate([s] * (wide // LANES), axis=1)
            r = s * mixed[g, 0, rows, :] + (1.0 - s) * mixed[g, 1, rows, :]
            mixed[g, 0, rows, :] = r
            return acc + jnp.sum((r * r).reshape(tile // 8, 8, wide), axis=0)

        acc = lax.fori_loop(0, depth // tile, mix, jnp.zeros((8, wide), jnp.float32))
        part[me, pl.ds(g, 1), :] = jnp.sum(acc, axis=0, keepdims=True)

    pl.semaphore_wait(barrier, n_rows - 1 + jnp.where(envoy, n_width - 1, 0))

    def to_others(ref, sems, axis, mine, size):
        for d in range(1, size):
            pltpu.make_async_remote_copy(
                src_ref=ref,
                dst_ref=ref,
                send_sem=sems.at[0],
                recv_sem=sems.at[1],
                device_id={axis: lax.rem(mine + d, size)},
                device_id_type=MESH,
            ).start()

    to_others(part.at[me], sum_sem, "rows", me, n_rows)

    cross_first, _ = split_groups(count)

    def bucket(g):
        return 2 * g // (count + 1)

    core = me % 2
    place = (me // 2) % CIRCLE
    side = me // (2 * CIRCLE)

    def device(sides, steps):
        return ((side + sides) % 2 * CIRCLE + (place + steps + CIRCLE) % CIRCLE) * 2 + core

    twin = me + 1 - 2 * core
    target = {UP: device(0, 1), DOWN: device(0, -1), ACROSS: device(1, 0)}
    def whole(owner):
        return pl.ds(pl.multiple_of(owner * depth, half), depth)

    def part_of(owner, way):
        return pl.ds(pl.multiple_of(owner * depth + way * half, half), half)

    def rows_of(item, sender):
        link, far, hop, _ = item
        if link == ACROSS:
            side_of = 0 if sender else 1
            if hop >= 3:
                return part_of(device(side_of, 2), hop - 3)
            return whole(device(side_of, (0, -1, 1)[hop]))
        away = hop - 1 if sender else hop
        owner = device(far, -away if link == UP else away)
        return whole(owner) if hop == 1 else part_of(owner, link)

    def remote(item, sender):
        link, far, hop, g = item
        ref = blocks[g].at[rows_of(item, sender), :]
        if link == ACROSS:
            arrived = pair_recv.at[hop, g]
        else:
            arrived = ring_recv.at[link, far, hop - 1, g]
        return pltpu.make_async_remote_copy(
            src_ref=ref,
            dst_ref=ref,
            send_sem=send_sem.at[link, bucket(g)],
            recv_sem=arrived,
            device_id={"rows": target[link]},
            device_id_type=MESH,
        )

    sent = {}

    def send(item):
        remote(item, True).start()
        link, _, hop, g = item
        key = link, bucket(g)
        sent[key] = sent.get(key, 0) + (depth if is_whole(item) else half)

    def share_with_twin(g, rows):
        ref = blocks[g].at[rows, :]
        pltpu.make_async_remote_copy(
            src_ref=ref,
            dst_ref=ref,
            send_sem=twin_sem.at[0, g],
            recv_sem=twin_sem.at[1, g],
            device_id={"rows": twin},
            device_id_type=MESH,
        ).start()

    others = part.at[pl.ds(0, n_rows - 1)]
    drain(others, sum_sem.at[1])
    total = part[0, pl.ds(0, count), :]
    for p in range(1, n_rows):
        total = total + part[p, pl.ds(0, count), :]
    scale = jnp.sqrt(total)
    inverse = 1.0 / scale

    def release(g):
        send((ACROSS, 0, 0, g))
        send((UP, 0, 1, g))
        send((DOWN, 0, 1, g))
        share_with_twin(g, whole(me))

    for g, (_, _, out, col, at) in enumerate(groups):
        col[pl.ds(at, wide)] = scale[g : g + 1, :].reshape(wide)
        by = inverse[g : g + 1, :]

        def narrow(i, carry):
            rows = pl.ds(pl.multiple_of(i * tile, tile), tile)
            here = pl.ds(pl.multiple_of(me * depth + i * tile, tile), tile)
            out[here, :] = (mixed[g, 0, rows, :] * by).astype(out.dtype)
            return carry

        lax.fori_loop(0, depth // tile, narrow, 0)
        if g:
            release(g - 1)
    release(count - 1)

    rows_half = n_rows // 2
    other_slabs = slab.at[pl.ds(0, n_width - 1)]

    @pl.when(envoy)
    def _():
        for p in range(n_rows):
            slab[lane, pl.ds(p % 2 * rows_half + p // 2, 1), :] = part[p, pl.ds(count, 1), :]
        to_others(slab.at[lane], slab_sem, "width", lane, n_width)

    def relay(way):
        return pltpu.make_async_remote_copy(
            src_ref=serve,
            dst_ref=serve,
            send_sem=relay_send.at[way],
            recv_sem=relay_recv.at[0],
            device_id={"rows": target.get(way, twin)},
            device_id_type=MESH,
        )

    def assemble():
        drain(other_slabs, slab_sem.at[1])
        per_line = 2 * n_width * piece_size
        at_lane = lax.broadcasted_iota(jnp.int32, (rows_half, LANES), 1)
        tiles = [jnp.zeros((rows_half, LANES), jnp.float32)] * (per_line // LANES)
        for k in range(2 * n_width):
            x = slab[k % n_width, pl.ds(k // n_width * rows_half, rows_half), :]
            t, o = divmod(k * piece_size, LANES)
            x = pltpu.roll(x, o, 1) if o else x
            end = o + piece_size
            tiles[t] = jnp.where((at_lane >= o) & (at_lane < end), x, tiles[t])
            if end > LANES:
                tiles[t + 1] = jnp.where(at_lane < end - LANES, x, tiles[t + 1])
        for t, x in enumerate(tiles):
            for a in range(rows_half):
                flat[pl.ds(a * per_line + t * LANES, LANES)] = x[a : a + 1, :].reshape(LANES)
        serve[...] = flat[...].astype(serve.dtype)

    TWIN = 3
    lead = core == 0
    duties = [
        (envoy, (UP, DOWN, ACROSS, TWIN)),
        (lead & (place == 0) & (side == 1), (UP, DOWN, TWIN)),
        (lead & (place == 1), (UP, TWIN)),
        (lead & (place == 3), (TWIN,)),
        (lead & (place == 2), (TWIN,)),
        (core == 1, ()),
    ]

    def duty(i):
        role, ways = duties[i]

        @pl.when(role)
        def _():
            if i == 0:
                assemble()
            else:
                drain(serve, relay_recv.at[0])
            for way in ways:
                relay(way).start()

    schedule = plan(count, cross_first)
    moments = [len(schedule) * (3 + i) // 12 for i in range(len(duties))]
    for index, (item, steps) in enumerate(schedule):
        if index in moments:
            duty(moments.index(index))
        g = item[3]
        remote(item, False).wait_recv()
        for step_on in steps:
            send(step_on)
        share_with_twin(g, rows_of(item, False))

    for (link, key), rows in sent.items():
        drain(blocks[0].at[pl.ds(0, rows), :], send_sem.at[link, key])
    for g, block in enumerate(blocks):
        for way in range(2):
            drain(block.at[pl.ds(0, depth * n_rows // 2), :], twin_sem.at[way, g])
    drain(others, sum_sem.at[0])
    for i, (role, ways) in enumerate(duties):

        @pl.when(role)
        def _(i=i, ways=ways):
            if i == 0:
                drain(other_slabs, slab_sem.at[0])
            for way in ways:
                relay(way).wait_send()


def store(*refs):
    outs, sem = refs[-8:-1], refs[-1]
    blocks, small = refs[:-12], refs[-12:-8]
    wide = blocks[0].shape[1]
    pairs = [(blocks[0], outs[1]), (blocks[1], outs[2])] + list(zip(small, outs[3:]))
    for j, block in enumerate(blocks[2:]):
        pairs.append((block, outs[0].at[:, pl.ds(j * wide, wide)]))
    copies = [pltpu.make_async_copy(src, dst, sem.at[i]) for i, (src, dst) in enumerate(pairs)]
    for copy in copies:
        copy.start()
    for copy in copies:
        copy.wait()


def solution(mesh):
    n_rows, n_width = mesh.shape["rows"], mesh.shape["width"]

    def shards(
        one_query,
        other_query,
        one_key,
        other_key,
        one_value,
        other_value,
        mix_share,
        norm_train,
        norm_step,
    ):
        depth, wide = one_key.shape
        wide_query = one_query.shape[1]
        count = 2 + wide_query // wide
        piece = norm_train.shape[0]
        total = depth * n_rows
        hbm = pl.BlockSpec(memory_space=pltpu.HBM)
        vmem = pl.BlockSpec(memory_space=pltpu.VMEM)
        dma = pltpu.SemaphoreType.DMA
        out_shape = (pltpu.VMEM((total, wide), jnp.bfloat16),) * count + (
            pltpu.VMEM((wide_query,), jnp.float32),
            pltpu.VMEM((wide,), jnp.float32),
            pltpu.VMEM((wide,), jnp.float32),
            pltpu.VMEM((n_rows * n_width * piece,), jnp.bfloat16),
        )
        gathered = pl.pallas_call(
            lambda *refs: kernel(n_rows, n_width, *refs),
            out_shape=out_shape,
            in_specs=[hbm] * 9,
            out_specs=[vmem] * (count + 4),
            scratch_shapes=[
                pltpu.VMEM((count, 2, depth, wide), jnp.float32),
                pltpu.VMEM((depth, LANES), jnp.float32),
                pltpu.VMEM((depth,), jnp.float32),
                pltpu.VMEM((piece,), jnp.float32),
                pltpu.VMEM((piece,), jnp.float32),
                pltpu.VMEM((n_rows, count + 1, wide), jnp.float32),
                pltpu.VMEM((n_width, n_rows, LANES), jnp.float32),
                pltpu.VMEM((n_rows * n_width * piece,), jnp.float32),
                dma((count,)),
                dma((3,)),
                dma((2,)),
                dma((4,)),
                dma((1,)),
                dma((2,)),
                dma((3, 2)),
                dma((2, 2, 2, count)),
                dma((5, count)),
                dma((2, count)),
            ],
            compiler_params=pltpu.CompilerParams(
                collective_id=0, has_side_effects=True, vmem_limit_bytes=44 * 1024 * 1024
            ),
        )(mix_share, norm_train, norm_step, one_query, other_query, one_key, other_key, one_value, other_value)
        return pl.pallas_call(
            store,
            out_shape=(
                jax.ShapeDtypeStruct((total, wide_query), jnp.bfloat16),
                jax.ShapeDtypeStruct((total, wide), jnp.bfloat16),
                jax.ShapeDtypeStruct((total, wide), jnp.bfloat16),
            )
            + tuple(jax.ShapeDtypeStruct(o.shape, o.dtype) for o in out_shape[count:]),
            in_specs=[vmem] * (count + 4),
            out_specs=[hbm] * 7,
            scratch_shapes=[dma((count + 4,))],
            compiler_params=pltpu.CompilerParams(vmem_limit_bytes=1024 * 1024),
        )(*gathered)

    wide_spec = P("rows", "width")
    in_specs = (wide_spec,) * 6 + (P("rows"), P(("rows", "width")), P(("rows", "width")))
    out_specs = (P(None, "width"),) * 3 + (P("width"),) * 3 + (P(),)
    return jax.shard_map(shards, mesh=mesh, in_specs=in_specs, out_specs=out_specs, check_vma=False)
```

```python
import jax
import jax.numpy as jnp
from jax import lax
from jax.experimental import pallas as pl
from jax.experimental.pallas import tpu as pltpu
from jax.sharding import PartitionSpec as P

MESH = pl.DeviceIdType.MESH
LANES = 128
CIRCLE = 4
UP, DOWN, ACROSS = 0, 1, 2
DEPTH = 9
LAG = 0.7


def split_groups(count):
    first = [g for g in range(count) if g % 2 == 0]
    return first, [g for g in range(count) if g % 2]


def plan(count, cross_first):
    free, flying, ready = [0.0] * 3, [0] * 3, [[], [], []]
    events, order, clock = [], [], [0]

    def put(now, event):
        clock[0] += 1
        events.append((now, clock[0], event))

    def offer(item):
        clock[0] += 1
        ready[item[0]].append((-steps_after(item, cross_first), clock[0], item))

    first = [g for g in range(count) if g in cross_first]
    second = [g for g in range(count) if g not in cross_first]
    for k in range(max(len(first), len(second))):
        for g in second[k : k + 1] + first[k : k + 1]:
            put(0.05 * len(events), g)
    while events:
        events.sort()
        now, _, event = events.pop(0)
        if isinstance(event, int):
            for item in ((ACROSS, 0, 0, event), (UP, 0, 1, event), (DOWN, 0, 1, event)):
                offer(item)
        else:
            flying[event[0]] -= 1
            for item in followers(event, cross_first):
                offer(item)
        sends = []
        for link in (ACROSS, UP, DOWN):
            ready[link].sort()
            while ready[link] and flying[link] < DEPTH:
                item = ready[link].pop(0)[2]
                flying[link] += 1
                free[link] = max(free[link], now) + (1.0 if is_whole(item) else 0.5)
                put(free[link] + LAG, item)
                sends.append(item)
        order.append((event, sends))
    return order


def steps_after(item, cross_first):
    return max([1 + steps_after(x, cross_first) for x in followers(item, cross_first)], default=0)


def is_whole(item):
    link, _, hop, _ = item
    return hop < 3 if link == ACROSS else hop == 1


def followers(item, cross_first):
    link, far, hop, g = item
    if link == ACROSS:
        return [(UP, 1, 1, g), (DOWN, 1, 1, g)] if g in cross_first else []
    steps = [(link, far, 2, g)] if hop == 1 else []
    if g not in cross_first:
        steps.append((ACROSS, 0, 1 + link if hop == 1 else 3 + link, g))
    return steps


def kernel(
    n_rows,
    n_width,
    share_in,
    norm_train,
    norm_step,
    one_query,
    other_query,
    one_key,
    other_key,
    one_value,
    other_value,
    *refs,
):
    blocks = refs[: 2 + one_query.shape[1] // one_key.shape[1]]
    col_query, col_key, col_value, serve, mixed, share = refs[len(blocks) :][:6]
    line, train, step, part, slab, flat, in_sem, small_sem = refs[len(blocks) + 6 :][:8]
    slab_sem, relay_send, relay_recv, sum_sem, send_sem = refs[len(blocks) + 14 :][:5]
    ring_recv, pair_recv, twin_sem = refs[len(blocks) + 19 :]
    me = lax.axis_index("rows")
    lane = lax.axis_index("width")
    depth, wide = one_key.shape
    groups = [
        (one_key, other_key, blocks[0], col_key, 0),
        (one_value, other_value, blocks[1], col_value, 0),
    ] + [
        (one_query, other_query, blocks[2 + j], col_query, j * wide)
        for j in range(one_query.shape[1] // wide)
    ]
    count = len(groups)
    tile = 64 if depth % 64 == 0 else 16
    half = depth // 2

    def drain(ref, sem):
        pltpu.make_async_copy(ref, ref, sem).wait()

    small = []
    for i, (src, dst) in enumerate(((share_in, line), (norm_train, train), (norm_step, step))):
        small.append(pltpu.make_async_copy(src, dst, small_sem.at[i]))
        small[-1].start()
    for g, (one, other, _, _, at) in enumerate(groups):
        a = pltpu.make_async_copy(one.at[:, pl.ds(at, wide)], mixed.at[g, 0], in_sem.at[g])
        b = pltpu.make_async_copy(other.at[:, pl.ds(at, wide)], mixed.at[g, 1], in_sem.at[g])
        a.start()
        b.start()

    barrier = pltpu.get_barrier_semaphore()
    for d in range(1, n_rows):
        pl.semaphore_signal(
            barrier, inc=1, device_id={"rows": lax.rem(me + d, n_rows)}, device_id_type=MESH
        )

    envoy = me == 0

    @pl.when(envoy)
    def _():
        for d in range(1, n_width):
            pl.semaphore_signal(
                barrier, inc=1, device_id={"width": lax.rem(lane + d, n_width)}, device_id_type=MESH
            )

    for copy in small:
        copy.wait()
    piece_size = norm_train.shape[0]
    part[me, pl.ds(count, 1), :] = jnp.zeros((1, wide), jnp.float32)
    part[me, pl.ds(count, 1), pl.ds(0, piece_size)] = (train[...] + step[...]).reshape(1, -1)
    for at in range(0, depth, LANES):
        size = min(LANES, depth - at)
        piece = line[pl.ds(at, size)].reshape(1, size)
        share[pl.ds(at, size), :] = jnp.broadcast_to(piece, (LANES, size)).T

    for g in range(count):
        drain(mixed.at[g], in_sem.at[g])

        def mix(i, acc):
            rows = pl.ds(pl.multiple_of(i * tile, tile), tile)
            s = share[rows, :]
            s = jnp.concatenate([s] * (wide // LANES), axis=1)
            r = s * mixed[g, 0, rows, :] + (1.0 - s) * mixed[g, 1, rows, :]
            mixed[g, 0, rows, :] = r
            return acc + jnp.sum((r * r).reshape(tile // 8, 8, wide), axis=0)

        acc = lax.fori_loop(0, depth // tile, mix, jnp.zeros((8, wide), jnp.float32))
        part[me, pl.ds(g, 1), :] = jnp.sum(acc, axis=0, keepdims=True)

    pl.semaphore_wait(barrier, n_rows - 1 + jnp.where(envoy, n_width - 1, 0))

    def to_others(ref, sems, axis, mine, size):
        for d in range(1, size):
            pltpu.make_async_remote_copy(
                src_ref=ref,
                dst_ref=ref,
                send_sem=sems.at[0],
                recv_sem=sems.at[1],
                device_id={axis: lax.rem(mine + d, size)},
                device_id_type=MESH,
            ).start()

    to_others(part.at[me], sum_sem, "rows", me, n_rows)

    cross_first, _ = split_groups(count)

    def bucket(g):
        return 2 * g // (count + 1)

    core = me % 2
    place = (me // 2) % CIRCLE
    side = me // (2 * CIRCLE)

    def device(sides, steps):
        return ((side + sides) % 2 * CIRCLE + (place + steps + CIRCLE) % CIRCLE) * 2 + core

    twin = me + 1 - 2 * core
    target = {UP: device(0, 1), DOWN: device(0, -1), ACROSS: device(1, 0)}
    def whole(owner):
        return pl.ds(pl.multiple_of(owner * depth, half), depth)

    def part_of(owner, way):
        return pl.ds(pl.multiple_of(owner * depth + way * half, half), half)

    def rows_of(item, sender):
        link, far, hop, _ = item
        if link == ACROSS:
            side_of = 0 if sender else 1
            if hop >= 3:
                return part_of(device(side_of, 2), hop - 3)
            return whole(device(side_of, (0, -1, 1)[hop]))
        away = hop - 1 if sender else hop
        owner = device(far, -away if link == UP else away)
        return whole(owner) if hop == 1 else part_of(owner, link)

    def remote(item, sender):
        link, far, hop, g = item
        ref = blocks[g].at[rows_of(item, sender), :]
        if link == ACROSS:
            arrived = pair_recv.at[hop, g]
        else:
            arrived = ring_recv.at[link, far, hop - 1, g]
        return pltpu.make_async_remote_copy(
            src_ref=ref,
            dst_ref=ref,
            send_sem=send_sem.at[link, bucket(g)],
            recv_sem=arrived,
            device_id={"rows": target[link]},
            device_id_type=MESH,
        )

    sent = {}

    def send(item):
        remote(item, True).start()
        link, _, hop, g = item
        key = link, bucket(g)
        sent[key] = sent.get(key, 0) + (depth if is_whole(item) else half)

    def share_with_twin(g, rows):
        ref = blocks[g].at[rows, :]
        pltpu.make_async_remote_copy(
            src_ref=ref,
            dst_ref=ref,
            send_sem=twin_sem.at[0, g],
            recv_sem=twin_sem.at[1, g],
            device_id={"rows": twin},
            device_id_type=MESH,
        ).start()

    others = part.at[pl.ds(0, n_rows - 1)]
    drain(others, sum_sem.at[1])
    total = part[0, pl.ds(0, count), :]
    for p in range(1, n_rows):
        total = total + part[p, pl.ds(0, count), :]
    scale = jnp.sqrt(total)
    inverse = 1.0 / scale

    def make_block(g):
        _, _, out, col, at = groups[g]
        col[pl.ds(at, wide)] = scale[g : g + 1, :].reshape(wide)
        by = inverse[g : g + 1, :]

        def narrow(i, carry):
            rows = pl.ds(pl.multiple_of(i * tile, tile), tile)
            here = pl.ds(pl.multiple_of(me * depth + i * tile, tile), tile)
            out[here, :] = (mixed[g, 0, rows, :] * by).astype(out.dtype)
            return carry

        lax.fori_loop(0, depth // tile, narrow, 0)

    rows_half = n_rows // 2
    other_slabs = slab.at[pl.ds(0, n_width - 1)]

    def meet():
        for p in range(n_rows):
            slab[lane, pl.ds(p % 2 * rows_half + p // 2, 1), :] = part[p, pl.ds(count, 1), :]
        to_others(slab.at[lane], slab_sem, "width", lane, n_width)

    def relay(way):
        return pltpu.make_async_remote_copy(
            src_ref=serve,
            dst_ref=serve,
            send_sem=relay_send.at[way],
            recv_sem=relay_recv.at[0],
            device_id={"rows": target.get(way, twin)},
            device_id_type=MESH,
        )

    def assemble():
        drain(other_slabs, slab_sem.at[1])
        per_line = 2 * n_width * piece_size
        at_lane = lax.broadcasted_iota(jnp.int32, (rows_half, LANES), 1)
        tiles = [jnp.zeros((rows_half, LANES), jnp.float32)] * (per_line // LANES)
        for k in range(2 * n_width):
            x = slab[k % n_width, pl.ds(k // n_width * rows_half, rows_half), :]
            t, o = divmod(k * piece_size, LANES)
            x = pltpu.roll(x, o, 1) if o else x
            end = o + piece_size
            tiles[t] = jnp.where((at_lane >= o) & (at_lane < end), x, tiles[t])
            if end > LANES:
                tiles[t + 1] = jnp.where(at_lane < end - LANES, x, tiles[t + 1])
        for t, x in enumerate(tiles):
            for a in range(rows_half):
                flat[pl.ds(a * per_line + t * LANES, LANES)] = x[a : a + 1, :].reshape(LANES)
        serve[...] = flat[...].astype(serve.dtype)

    TWIN = 3
    lead = core == 0
    duties = [
        (envoy, (UP, DOWN, ACROSS, TWIN)),
        (lead & (place == 0) & (side == 1), (UP, DOWN, TWIN)),
        (lead & (place == 1), (UP, TWIN)),
        (lead & (place == 3), (TWIN,)),
        (lead & (place == 2), (TWIN,)),
        (core == 1, ()),
    ]

    def duty(i):
        role, ways = duties[i]

        @pl.when(role)
        def _():
            if i == 0:
                assemble()
            else:
                drain(serve, relay_recv.at[0])
            for way in ways:
                relay(way).start()

    schedule = plan(count, cross_first)
    moments = [len(schedule) * (3 + i) // 12 for i in range(len(duties))]
    for index, (event, items) in enumerate(schedule):
        if index == count:
            pl.when(envoy)(meet)
        if index in moments:
            duty(moments.index(index))
        if isinstance(event, int):
            make_block(event)
            g, rows = event, whole(me)
        else:
            remote(event, False).wait_recv()
            g, rows = event[3], rows_of(event, False)
        for item in items:
            send(item)
        share_with_twin(g, rows)

    for (link, key), rows in sent.items():
        drain(blocks[0].at[pl.ds(0, rows), :], send_sem.at[link, key])
    for g, block in enumerate(blocks):
        for way in range(2):
            drain(block.at[pl.ds(0, depth * n_rows // 2), :], twin_sem.at[way, g])
    drain(others, sum_sem.at[0])
    for i, (role, ways) in enumerate(duties):

        @pl.when(role)
        def _(i=i, ways=ways):
            if i == 0:
                drain(other_slabs, slab_sem.at[0])
            for way in ways:
                relay(way).wait_send()


def store(*refs):
    outs, sem = refs[-8:-1], refs[-1]
    blocks, small = refs[:-12], refs[-12:-8]
    wide = blocks[0].shape[1]
    pairs = [(blocks[0], outs[1]), (blocks[1], outs[2])] + list(zip(small, outs[3:]))
    for j, block in enumerate(blocks[2:]):
        pairs.append((block, outs[0].at[:, pl.ds(j * wide, wide)]))
    copies = [pltpu.make_async_copy(src, dst, sem.at[i]) for i, (src, dst) in enumerate(pairs)]
    for copy in copies:
        copy.start()
    for copy in copies:
        copy.wait()


def solution(mesh):
    n_rows, n_width = mesh.shape["rows"], mesh.shape["width"]

    def shards(
        one_query,
        other_query,
        one_key,
        other_key,
        one_value,
        other_value,
        mix_share,
        norm_train,
        norm_step,
    ):
        depth, wide = one_key.shape
        wide_query = one_query.shape[1]
        count = 2 + wide_query // wide
        piece = norm_train.shape[0]
        total = depth * n_rows
        hbm = pl.BlockSpec(memory_space=pltpu.HBM)
        vmem = pl.BlockSpec(memory_space=pltpu.VMEM)
        dma = pltpu.SemaphoreType.DMA
        out_shape = (pltpu.VMEM((total, wide), jnp.bfloat16),) * count + (
            pltpu.VMEM((wide_query,), jnp.float32),
            pltpu.VMEM((wide,), jnp.float32),
            pltpu.VMEM((wide,), jnp.float32),
            pltpu.VMEM((n_rows * n_width * piece,), jnp.bfloat16),
        )
        gathered = pl.pallas_call(
            lambda *refs: kernel(n_rows, n_width, *refs),
            out_shape=out_shape,
            in_specs=[hbm] * 9,
            out_specs=[vmem] * (count + 4),
            scratch_shapes=[
                pltpu.VMEM((count, 2, depth, wide), jnp.float32),
                pltpu.VMEM((depth, LANES), jnp.float32),
                pltpu.VMEM((depth,), jnp.float32),
                pltpu.VMEM((piece,), jnp.float32),
                pltpu.VMEM((piece,), jnp.float32),
                pltpu.VMEM((n_rows, count + 1, wide), jnp.float32),
                pltpu.VMEM((n_width, n_rows, LANES), jnp.float32),
                pltpu.VMEM((n_rows * n_width * piece,), jnp.float32),
                dma((count,)),
                dma((3,)),
                dma((2,)),
                dma((4,)),
                dma((1,)),
                dma((2,)),
                dma((3, 2)),
                dma((2, 2, 2, count)),
                dma((5, count)),
                dma((2, count)),
            ],
            compiler_params=pltpu.CompilerParams(
                collective_id=0, has_side_effects=True, vmem_limit_bytes=44 * 1024 * 1024
            ),
        )(mix_share, norm_train, norm_step, one_query, other_query, one_key, other_key, one_value, other_value)
        return pl.pallas_call(
            store,
            out_shape=(
                jax.ShapeDtypeStruct((total, wide_query), jnp.bfloat16),
                jax.ShapeDtypeStruct((total, wide), jnp.bfloat16),
                jax.ShapeDtypeStruct((total, wide), jnp.bfloat16),
            )
            + tuple(jax.ShapeDtypeStruct(o.shape, o.dtype) for o in out_shape[count:]),
            in_specs=[vmem] * (count + 4),
            out_specs=[hbm] * 7,
            scratch_shapes=[dma((count + 4,))],
            compiler_params=pltpu.CompilerParams(vmem_limit_bytes=1024 * 1024),
        )(*gathered)

    wide_spec = P("rows", "width")
    in_specs = (wide_spec,) * 6 + (P("rows"), P(("rows", "width")), P(("rows", "width")))
    out_specs = (P(None, "width"),) * 3 + (P("width"),) * 3 + (P(),)
    return jax.shard_map(shards, mesh=mesh, in_specs=in_specs, out_specs=out_specs, check_vma=False)
```

```python
import jax
import jax.numpy as jnp
from jax import lax
from jax.experimental import pallas as pl
from jax.experimental.pallas import tpu as pltpu
from jax.sharding import PartitionSpec as P

MESH = pl.DeviceIdType.MESH
LANES = 128
CIRCLE = 4
UP, DOWN, ACROSS = 0, 1, 2
SPAN = 2
WINDOW = 4
DEPTH = 9
LAG = 0.7


def layout(count):
    first = (5 * count + 4) // 9

    def cut(start, end):
        return [list(range(i, min(i + SPAN, end))) for i in range(start, end, SPAN)]

    blocks = cut(0, first) + cut(first, count)
    return blocks, [b for b, pieces in enumerate(blocks) if pieces[0] < first]


def plan(weights, cross_first):
    free, flying, ready = [0.0] * 3, [0] * 3, [[], [], []]
    events, order, clock = [], [], [0]

    def put(now, event):
        clock[0] += 1
        events.append((now, clock[0], event))

    def offer(item):
        clock[0] += 1
        ready[item[0]].append((-steps_after(item, cross_first), clock[0], item))

    first = cross_first
    second = [b for b in range(len(weights)) if b not in cross_first]
    for k in range(max(len(first), len(second))):
        for b in second[k : k + 1] + first[k : k + 1]:
            put(0.1 * len(events), b)
    while events:
        events.sort()
        now, _, event = events.pop(0)
        if isinstance(event, int):
            for item in ((ACROSS, 0, 0, event), (UP, 0, 1, event), (DOWN, 0, 1, event)):
                offer(item)
        else:
            flying[event[0]] -= 1
            for item in followers(event, cross_first):
                offer(item)
        sends = []
        for link in (ACROSS, UP, DOWN):
            ready[link].sort()
            while ready[link] and flying[link] < DEPTH:
                item = ready[link].pop(0)[2]
                flying[link] += 1
                size = weights[item[3]] * (1.0 if is_whole(item) else 0.5)
                free[link] = max(free[link], now) + size
                put(free[link] + LAG, item)
                sends.append(item)
        order.append((event, sends))
    return order


def steps_after(item, cross_first):
    return max([1 + steps_after(x, cross_first) for x in followers(item, cross_first)], default=0)


def is_whole(item):
    link, _, hop, _ = item
    return hop < 3 if link == ACROSS else hop == 1


def followers(item, cross_first):
    link, far, hop, g = item
    if link == ACROSS:
        return [(UP, 1, 1, g), (DOWN, 1, 1, g)] if g in cross_first else []
    steps = [(link, far, 2, g)] if hop == 1 else []
    if g not in cross_first:
        steps.append((ACROSS, 0, 1 + link if hop == 1 else 3 + link, g))
    return steps


def kernel(
    n_rows,
    n_width,
    pieces_of,
    cross_first,
    share_in,
    norm_train,
    norm_step,
    one_query,
    other_query,
    one_key,
    other_key,
    one_value,
    other_value,
    *refs,
):
    blocks = refs[: len(pieces_of)]
    col_query, col_key, col_value, serve, mixed, share = refs[len(blocks) :][:6]
    line, train, step, early_part, part, slab, flat = refs[len(blocks) + 6 :][:7]
    in_sem, small_sem, slab_sem, relay_send, relay_recv = refs[len(blocks) + 13 :][:5]
    early_sem, sum_sem, send_sem, ring_recv, pair_recv, twin_sem = refs[len(blocks) + 18 :]
    me = lax.axis_index("rows")
    lane = lax.axis_index("width")
    depth, wide = one_key.shape
    groups = [
        (one_key, other_key, col_key, 0),
        (one_value, other_value, col_value, 0),
    ] + [
        (one_query, other_query, col_query, j * wide)
        for j in range(one_query.shape[1] // wide)
    ]
    count = len(groups)
    tile = 64 if depth % 64 == 0 else 16
    half = depth // 2

    def drain(ref, sem):
        pltpu.make_async_copy(ref, ref, sem).wait()

    small = []
    for i, (src, dst) in enumerate(((share_in, line), (norm_train, train), (norm_step, step))):
        small.append(pltpu.make_async_copy(src, dst, small_sem.at[i]))
        small[-1].start()

    kinds = [cross_first, [b for b in range(len(blocks)) if b not in cross_first]]
    early = [p for kind in kinds for p in pieces_of[kind[0]]]
    late = [p for p in range(count) if p not in early]
    loading = early + late
    parts = {p: (early_part, k) for k, p in enumerate(early)}
    parts.update({p: (part, k) for k, p in enumerate(late)})

    def load(p):
        one, other, _, at = groups[p]
        for i, src in enumerate((one, other)):
            src = src.at[:, pl.ds(at, wide)]
            pltpu.make_async_copy(src, mixed.at[p, i], in_sem.at[p]).start()

    for p in loading[:WINDOW]:
        load(p)

    barrier = pltpu.get_barrier_semaphore()
    for d in range(1, n_rows):
        pl.semaphore_signal(
            barrier, inc=1, device_id={"rows": lax.rem(me + d, n_rows)}, device_id_type=MESH
        )

    envoy = me == 0
    row = n_width // 2
    along = [lane // row * row + (lane + d) % row for d in range(1, row)]
    opposite = (lane + row) % n_width

    @pl.when(envoy)
    def _():
        for peer in along + [opposite]:
            pl.semaphore_signal(barrier, inc=1, device_id={"width": peer}, device_id_type=MESH)

    for copy in small:
        copy.wait()
    piece_size = norm_train.shape[0]
    norm_at = pl.ds(len(late), 1)
    part[me, norm_at, :] = jnp.zeros((1, wide), jnp.float32)
    part[me, norm_at, pl.ds(0, piece_size)] = (train[...] + step[...]).reshape(1, -1)
    for at in range(0, depth, LANES):
        size = min(LANES, depth - at)
        piece = line[pl.ds(at, size)].reshape(1, size)
        share[pl.ds(at, size), :] = jnp.broadcast_to(piece, (LANES, size)).T

    core = me % 2
    place = (me // 2) % CIRCLE
    side = me // (2 * CIRCLE)

    def device(sides, steps, cores=0):
        chip = (side + sides) % 2 * CIRCLE + (place + steps + CIRCLE) % CIRCLE
        return chip * 2 + (core + cores) % 2

    far = [(a, b, c) for b in (2, 1, -1, 0) for a in (1, 0) for c in (1, 0) if (a, b, c) != (0, 0, 0)]

    def sum_up(p):
        drain(mixed.at[p], in_sem.at[p])
        if loading.index(p) + WINDOW < count:
            load(loading[loading.index(p) + WINDOW])

        def mix(i, acc):
            rows = pl.ds(pl.multiple_of(i * tile, tile), tile)
            s = share[rows, :]
            s = jnp.concatenate([s] * (wide // LANES), axis=1)
            r = s * mixed[p, 0, rows, :] + (1.0 - s) * mixed[p, 1, rows, :]
            mixed[p, 0, rows, :] = r
            return acc + jnp.sum((r * r).reshape(tile // 8, 8, wide), axis=0)

        acc = lax.fori_loop(0, depth // tile, mix, jnp.zeros((8, wide), jnp.float32))
        into, at_row = parts[p]
        into[me, pl.ds(at_row, 1), :] = jnp.sum(acc, axis=0, keepdims=True)

    def to_group(ref, sems):
        for where in far:
            pltpu.make_async_remote_copy(
                src_ref=ref.at[me],
                dst_ref=ref.at[me],
                send_sem=sems.at[0],
                recv_sem=sems.at[1],
                device_id={"rows": device(*where)},
                device_id_type=MESH,
            ).start()

    for p in early:
        sum_up(p)
    pl.semaphore_wait(barrier, n_rows - 1 + jnp.where(envoy, row, 0))
    to_group(early_part, early_sem)
    for p in late:
        sum_up(p)
    to_group(part, sum_sem)

    twin = me + 1 - 2 * core
    target = {UP: device(0, 1), DOWN: device(0, -1), ACROSS: device(1, 0)}
    def whole(owner):
        return pl.ds(pl.multiple_of(owner * depth, half), depth)

    def part_of(owner, way):
        return pl.ds(pl.multiple_of(owner * depth + way * half, half), half)

    def rows_of(item, sender):
        link, far, hop, _ = item
        if link == ACROSS:
            side_of = 0 if sender else 1
            if hop >= 3:
                return part_of(device(side_of, 2), hop - 3)
            return whole(device(side_of, (0, -1, 1)[hop]))
        away = hop - 1 if sender else hop
        owner = device(far, -away if link == UP else away)
        return whole(owner) if hop == 1 else part_of(owner, link)

    def remote(item, sender):
        link, far, hop, g = item
        ref = blocks[g].at[rows_of(item, sender), :]
        if link == ACROSS:
            arrived = pair_recv.at[hop, g]
        else:
            arrived = ring_recv.at[link, far, hop - 1, g]
        return pltpu.make_async_remote_copy(
            src_ref=ref,
            dst_ref=ref,
            send_sem=send_sem.at[link, g],
            recv_sem=arrived,
            device_id={"rows": target[link]},
            device_id_type=MESH,
        )

    sent = {}

    def send(item):
        remote(item, True).start()
        key = item[0], item[3]
        sent[key] = sent.get(key, 0) + (depth if is_whole(item) else half)

    def share_with_twin(g, rows):
        ref = blocks[g].at[rows, :]
        pltpu.make_async_remote_copy(
            src_ref=ref,
            dst_ref=ref,
            send_sem=twin_sem.at[0, g],
            recv_sem=twin_sem.at[1, g],
            device_id={"rows": twin},
            device_id_type=MESH,
        ).start()

    def scales(ref, sems, size):
        drain(ref.at[pl.ds(0, n_rows - 1)], sems.at[1])
        total = ref[0, pl.ds(0, size), :]
        for d in range(1, n_rows):
            total = total + ref[d, pl.ds(0, size), :]
        scale = jnp.sqrt(total)
        return scale, 1.0 / scale

    early_scales = scales(early_part, early_sem, len(early))
    late_scales = None

    def make_block(g):
        pieces, out = pieces_of[g], blocks[g]
        scale, inverse = early_scales if pieces[0] in early else late_scales
        for p in pieces:
            _, _, col, at = groups[p]
            at_row = parts[p][1]
            col[pl.ds(at, wide)] = scale[at_row : at_row + 1, :].reshape(wide)

        def narrow(i, carry):
            rows = pl.ds(pl.multiple_of(i * tile, tile), tile)
            here = pl.ds(pl.multiple_of(me * depth + i * tile, tile), tile)
            for j, p in enumerate(pieces):
                at_row = parts[p][1]
                made = mixed[p, 0, rows, :] * inverse[at_row : at_row + 1, :]
                out[here, pl.ds(j * wide, wide)] = made.astype(out.dtype)
            return carry

        lax.fori_loop(0, depth // tile, narrow, 0)

    rows_half = n_rows // 2

    def meet():
        for d in range(n_rows):
            slab[lane, pl.ds(d % 2 * rows_half + d // 2, 1), :] = part[d, norm_at, :]
        for peer in along:
            pltpu.make_async_remote_copy(
                src_ref=slab.at[lane],
                dst_ref=slab.at[lane],
                send_sem=slab_sem.at[0, 0],
                recv_sem=slab_sem.at[0, 1],
                device_id={"width": peer},
                device_id_type=MESH,
            ).start()

    def swap():
        drain(slab.at[pl.ds(0, row - 1)], slab_sem.at[0, 1])
        mine = slab.at[pl.ds(lane // row * row, row)]
        pltpu.make_async_remote_copy(
            src_ref=mine,
            dst_ref=mine,
            send_sem=slab_sem.at[1, 0],
            recv_sem=slab_sem.at[1, 1],
            device_id={"width": opposite},
            device_id_type=MESH,
        ).start()

    def relay(way):
        return pltpu.make_async_remote_copy(
            src_ref=serve,
            dst_ref=serve,
            send_sem=relay_send.at[way],
            recv_sem=relay_recv.at[0],
            device_id={"rows": target.get(way, twin)},
            device_id_type=MESH,
        )

    def assemble():
        drain(slab.at[pl.ds(0, row)], slab_sem.at[1, 1])
        per_line = 2 * n_width * piece_size
        at_lane = lax.broadcasted_iota(jnp.int32, (rows_half, LANES), 1)
        tiles = [jnp.zeros((rows_half, LANES), jnp.float32)] * (per_line // LANES)
        for k in range(2 * n_width):
            x = slab[k % n_width, pl.ds(k // n_width * rows_half, rows_half), :]
            t, o = divmod(k * piece_size, LANES)
            x = pltpu.roll(x, o, 1) if o else x
            end = o + piece_size
            tiles[t] = jnp.where((at_lane >= o) & (at_lane < end), x, tiles[t])
            if end > LANES:
                tiles[t + 1] = jnp.where(at_lane < end - LANES, x, tiles[t + 1])
        for t, x in enumerate(tiles):
            for a in range(rows_half):
                flat[pl.ds(a * per_line + t * LANES, LANES)] = x[a : a + 1, :].reshape(LANES)
        serve[...] = flat[...].astype(serve.dtype)

    TWIN = 3
    lead = core == 0
    duties = [
        (envoy, (UP, DOWN, ACROSS, TWIN)),
        (lead & (place == 0) & (side == 1), (UP, DOWN, TWIN)),
        (lead & (place == 1), (UP, TWIN)),
        (lead & (place == 3), (TWIN,)),
        (lead & (place == 2), (TWIN,)),
        (core == 1, ()),
    ]

    def duty(i):
        role, ways = duties[i]

        @pl.when(role)
        def _():
            if i == 0:
                assemble()
            else:
                drain(serve, relay_recv.at[0])
            for way in ways:
                relay(way).start()

    schedule = plan([len(pieces) for pieces in pieces_of], cross_first)
    moments = [len(schedule) * (3 + i) // 12 for i in range(len(duties))]
    meeting, swapping = len(blocks), (len(blocks) + moments[0]) // 2
    for index, (event, items) in enumerate(schedule):
        if index == meeting:
            pl.when(envoy)(meet)
        if index == swapping:
            pl.when(envoy)(swap)
        if index in moments:
            duty(moments.index(index))
        if isinstance(event, int):
            if late_scales is None and pieces_of[event][0] in late:
                late_scales = scales(part, sum_sem, len(late))
            make_block(event)
            g, rows = event, whole(me)
        else:
            remote(event, False).wait_recv()
            g, rows = event[3], rows_of(event, False)
        for item in items:
            send(item)
        share_with_twin(g, rows)

    for (link, key), rows in sent.items():
        drain(blocks[key].at[pl.ds(0, rows), :], send_sem.at[link, key])
    for g, block in enumerate(blocks):
        for way in range(2):
            drain(block.at[pl.ds(0, depth * n_rows // 2), :], twin_sem.at[way, g])
    drain(early_part.at[pl.ds(0, n_rows - 1)], early_sem.at[0])
    drain(part.at[pl.ds(0, n_rows - 1)], sum_sem.at[0])
    for i, (role, ways) in enumerate(duties):

        @pl.when(role)
        def _(i=i, ways=ways):
            if i == 0:
                drain(slab.at[pl.ds(0, row - 1)], slab_sem.at[0, 0])
                drain(slab.at[pl.ds(0, row)], slab_sem.at[1, 0])
            for way in ways:
                relay(way).wait_send()


def store(pieces_of, wide, *refs):
    outs, sem = refs[-8:-1], refs[-1]
    blocks, small = refs[:-12], refs[-12:-8]
    pairs = list(zip(small, outs[3:]))
    for pieces, block in zip(pieces_of, blocks):
        lone = [p for p in pieces if p < 2]
        for j, p in enumerate(lone):
            pairs.append((block.at[:, pl.ds(j * wide, wide)], outs[1 + p]))
        if pieces[len(lone) :]:
            at, size = (pieces[len(lone)] - 2) * wide, (len(pieces) - len(lone)) * wide
            pairs.append((block.at[:, pl.ds(len(lone) * wide, size)], outs[0].at[:, pl.ds(at, size)]))
    copies = [pltpu.make_async_copy(src, dst, sem.at[i]) for i, (src, dst) in enumerate(pairs)]
    for copy in copies:
        copy.start()
    for copy in copies:
        copy.wait()


def solution(mesh):
    n_rows, n_width = mesh.shape["rows"], mesh.shape["width"]

    def shards(
        one_query,
        other_query,
        one_key,
        other_key,
        one_value,
        other_value,
        mix_share,
        norm_train,
        norm_step,
    ):
        depth, wide = one_key.shape
        wide_query = one_query.shape[1]
        count = 2 + wide_query // wide
        pieces_of, cross_first = layout(count)
        n_blocks = len(pieces_of)
        n_early = len(pieces_of[0]) + len(pieces_of[len(cross_first)])
        piece = norm_train.shape[0]
        total = depth * n_rows
        hbm = pl.BlockSpec(memory_space=pltpu.HBM)
        vmem = pl.BlockSpec(memory_space=pltpu.VMEM)
        dma = pltpu.SemaphoreType.DMA
        out_shape = tuple(
            pltpu.VMEM((total, wide * len(pieces)), jnp.bfloat16) for pieces in pieces_of
        ) + (
            pltpu.VMEM((wide_query,), jnp.float32),
            pltpu.VMEM((wide,), jnp.float32),
            pltpu.VMEM((wide,), jnp.float32),
            pltpu.VMEM((n_rows * n_width * piece,), jnp.bfloat16),
        )
        gathered = pl.pallas_call(
            lambda *refs: kernel(n_rows, n_width, pieces_of, cross_first, *refs),
            out_shape=out_shape,
            in_specs=[hbm] * 9,
            out_specs=[vmem] * (n_blocks + 4),
            scratch_shapes=[
                pltpu.VMEM((count, 2, depth, wide), jnp.float32),
                pltpu.VMEM((depth, LANES), jnp.float32),
                pltpu.VMEM((depth,), jnp.float32),
                pltpu.VMEM((piece,), jnp.float32),
                pltpu.VMEM((piece,), jnp.float32),
                pltpu.VMEM((n_rows, n_early, wide), jnp.float32),
                pltpu.VMEM((n_rows, count - n_early + 1, wide), jnp.float32),
                pltpu.VMEM((n_width, n_rows, LANES), jnp.float32),
                pltpu.VMEM((n_rows * n_width * piece,), jnp.float32),
                dma((count,)),
                dma((3,)),
                dma((2, 2)),
                dma((4,)),
                dma((1,)),
                dma((2,)),
                dma((2,)),
                dma((3, n_blocks)),
                dma((2, 2, 2, n_blocks)),
                dma((5, n_blocks)),
                dma((2, n_blocks)),
            ],
            compiler_params=pltpu.CompilerParams(
                collective_id=0, has_side_effects=True, vmem_limit_bytes=44 * 1024 * 1024
            ),
        )(mix_share, norm_train, norm_step, one_query, other_query, one_key, other_key, one_value, other_value)
        return pl.pallas_call(
            lambda *refs: store(pieces_of, wide, *refs),
            out_shape=(
                jax.ShapeDtypeStruct((total, wide_query), jnp.bfloat16),
                jax.ShapeDtypeStruct((total, wide), jnp.bfloat16),
                jax.ShapeDtypeStruct((total, wide), jnp.bfloat16),
            )
            + tuple(jax.ShapeDtypeStruct(o.shape, o.dtype) for o in out_shape[n_blocks:]),
            in_specs=[vmem] * (n_blocks + 4),
            out_specs=[hbm] * 7,
            scratch_shapes=[dma((count + 4,))],
            compiler_params=pltpu.CompilerParams(vmem_limit_bytes=1024 * 1024),
        )(*gathered)

    wide_spec = P("rows", "width")
    in_specs = (wide_spec,) * 6 + (P("rows"), P(("rows", "width")), P(("rows", "width")))
    out_specs = (P(None, "width"),) * 3 + (P("width"),) * 3 + (P(),)
    return jax.shard_map(shards, mesh=mesh, in_specs=in_specs, out_specs=out_specs, check_vma=False)
```

```python
import jax
import jax.numpy as jnp
from jax import lax
from jax.experimental import pallas as pl
from jax.experimental.pallas import tpu as pltpu
from jax.sharding import PartitionSpec as P

MESH = pl.DeviceIdType.MESH
LANES = 128
CIRCLE = 4
UP, DOWN, ACROSS = 0, 1, 2
SPAN = 2
WINDOW = 4
DEPTH = 9
LAG = 0.7


def layout(count):
    first = (5 * count + 4) // 9

    def cut(start, end):
        return [list(range(i, min(i + SPAN, end))) for i in range(start, end, SPAN)]

    blocks = cut(0, first) + cut(first, count)
    return blocks, [b for b, pieces in enumerate(blocks) if pieces[0] < first]


def ahead_of(blocks, cross_first):
    last = cross_first[-1]
    return {(UP, 0, 1, last): 0, (DOWN, 0, 1, last): 1, (ACROSS, 0, 0, last): 0}


def plan(weights, cross_first, ahead):
    free, flying, ready = [0.0] * 3, [0] * 3, [[], [], []]
    events, order, clock = [], [], [0]

    def put(now, event):
        clock[0] += 1
        events.append((now, clock[0], event))

    def offer(item):
        clock[0] += 1
        ready[item[0]].append((-steps_after(item, cross_first), clock[0], item))

    first = cross_first
    second = [b for b in range(len(weights)) if b not in cross_first]
    for k in range(max(len(first), len(second))):
        for b in second[k : k + 1] + first[k : k + 1]:
            put(0.1 * len(events), b)
    while events:
        events.sort()
        now, _, event = events.pop(0)
        if isinstance(event, int):
            for item in ((ACROSS, 0, 0, event), (UP, 0, 1, event), (DOWN, 0, 1, event)):
                offer(item)
        else:
            flying[event[0]] -= 1
            for item in followers(event, cross_first):
                offer(item)
        sends = []
        for link in (ACROSS, UP, DOWN):
            ready[link].sort()
            while ready[link] and flying[link] < DEPTH:
                item = ready[link].pop(0)[2]
                flying[link] += 1
                size = weights[item[3]] * (1.0 if is_whole(item) and item not in ahead else 0.5)
                free[link] = max(free[link], now) + size
                put(free[link] + LAG, item)
                sends.append(item)
        order.append((event, sends))
    return order


def steps_after(item, cross_first):
    return max([1 + steps_after(x, cross_first) for x in followers(item, cross_first)], default=0)


def is_whole(item):
    link, _, hop, _ = item
    return hop < 3 if link == ACROSS else hop == 1


def followers(item, cross_first):
    link, far, hop, g = item
    if link == ACROSS:
        return [(UP, 1, 1, g), (DOWN, 1, 1, g)] if g in cross_first else []
    steps = [(link, far, 2, g)] if hop == 1 else []
    if g not in cross_first:
        steps.append((ACROSS, 0, 1 + link if hop == 1 else 3 + link, g))
    return steps


def kernel(
    n_rows,
    n_width,
    pieces_of,
    cross_first,
    ahead,
    schedule,
    share_in,
    norm_train,
    norm_step,
    one_query,
    other_query,
    one_key,
    other_key,
    one_value,
    other_value,
    *refs,
):
    blocks = refs[: len(pieces_of)]
    col_query, col_key, col_value, serve, mixed, share = refs[len(blocks) :][:6]
    line, train, step, early_part, part, slab, flat = refs[len(blocks) + 6 :][:7]
    in_sem, small_sem, slab_sem, relay_send, relay_recv = refs[len(blocks) + 13 :][:5]
    early_sem, sum_sem, send_sem, recv_sem, twin_sem = refs[len(blocks) + 18 :][:5]
    stage, stage_sem = refs[len(blocks) + 23 :]
    me = lax.axis_index("rows")
    lane = lax.axis_index("width")
    depth, wide = one_key.shape
    groups = [
        (one_key, other_key, col_key, 0),
        (one_value, other_value, col_value, 0),
    ] + [
        (one_query, other_query, col_query, j * wide)
        for j in range(one_query.shape[1] // wide)
    ]
    count = len(groups)
    tile = 64 if depth % 64 == 0 else 16
    half = depth // 2
    step_rows = 32 if half % 32 == 0 else 16

    def drain(ref, sem):
        pltpu.make_async_copy(ref, ref, sem).wait()

    small = []
    for i, (src, dst) in enumerate(((share_in, line), (norm_train, train), (norm_step, step))):
        small.append(pltpu.make_async_copy(src, dst, small_sem.at[i]))
        small[-1].start()

    kinds = [cross_first, [b for b in range(len(blocks)) if b not in cross_first]]
    early = [p for kind in kinds for p in pieces_of[kind[0]]]
    (first_out,) = pieces_of[cross_first[-1]]
    late = [first_out] + [p for p in range(count) if p not in early + [first_out]]
    loading = early + late
    parts = {p: (early_part, k) for k, p in enumerate(early)}
    parts.update({p: (part, k) for k, p in enumerate(late)})

    def load(p):
        one, other, _, at = groups[p]
        for i, src in enumerate((one, other)):
            src = src.at[:, pl.ds(at, wide)]
            pltpu.make_async_copy(src, mixed.at[p, i], in_sem.at[p]).start()

    for p in loading[:WINDOW]:
        load(p)

    barrier = pltpu.get_barrier_semaphore()
    for d in range(1, n_rows):
        pl.semaphore_signal(
            barrier, inc=1, device_id={"rows": lax.rem(me + d, n_rows)}, device_id_type=MESH
        )

    envoy = me == 0
    row = n_width // 2
    along = [lane // row * row + (lane + d) % row for d in range(1, row)]
    opposite = (lane + row) % n_width

    @pl.when(envoy)
    def _():
        for peer in along + [opposite]:
            pl.semaphore_signal(barrier, inc=1, device_id={"width": peer}, device_id_type=MESH)

    for copy in small:
        copy.wait()
    piece_size = norm_train.shape[0]
    norm_at = pl.ds(len(late), 1)
    part[me, norm_at, :] = jnp.zeros((1, wide), jnp.float32)
    part[me, norm_at, pl.ds(0, piece_size)] = (train[...] + step[...]).reshape(1, -1)
    for at in range(0, depth, LANES):
        size = min(LANES, depth - at)
        piece = line[pl.ds(at, size)].reshape(1, size)
        share[pl.ds(at, size), :] = jnp.broadcast_to(piece, (LANES, size)).T

    core = me % 2
    place = (me // 2) % CIRCLE
    side = me // (2 * CIRCLE)

    def device(sides, steps, cores=0):
        chip = (side + sides) % 2 * CIRCLE + (place + steps + CIRCLE) % CIRCLE
        return chip * 2 + (core + cores) % 2

    far = [(a, b, c) for b in (2, 1, -1, 0) for a in (1, 0) for c in (1, 0) if (a, b, c) != (0, 0, 0)]

    def sum_up(p):
        drain(mixed.at[p], in_sem.at[p])
        if loading.index(p) + WINDOW < count:
            load(loading[loading.index(p) + WINDOW])

        def mix(i, acc):
            rows = pl.ds(pl.multiple_of(i * tile, tile), tile)
            s = share[rows, :]
            s = jnp.concatenate([s] * (wide // LANES), axis=1)
            r = s * mixed[p, 0, rows, :] + (1.0 - s) * mixed[p, 1, rows, :]
            mixed[p, 0, rows, :] = r
            return acc + jnp.sum((r * r).reshape(tile // 8, 8, wide), axis=0)

        acc = lax.fori_loop(0, depth // tile, mix, jnp.zeros((8, wide), jnp.float32))
        into, at_row = parts[p]
        into[me, pl.ds(at_row, 1), :] = jnp.sum(acc, axis=0, keepdims=True)

    def to_group(ref, sems):
        for where in far:
            pltpu.make_async_remote_copy(
                src_ref=ref.at[me],
                dst_ref=ref.at[me],
                send_sem=sems.at[0],
                recv_sem=sems.at[1],
                device_id={"rows": device(*where)},
                device_id_type=MESH,
            ).start()

    for p in early:
        sum_up(p)
    pl.semaphore_wait(barrier, n_rows - 1 + jnp.where(envoy, row, 0))
    to_group(early_part, early_sem)
    twin = me + 1 - 2 * core
    target = {UP: device(0, 1), DOWN: device(0, -1), ACROSS: device(1, 0)}
    sum_up(first_out)
    for item, way in ahead.items():
        pltpu.make_async_remote_copy(
            src_ref=mixed.at[first_out, 0, pl.ds(way * half, half), :],
            dst_ref=stage.at[item[0]],
            send_sem=stage_sem.at[0, item[0]],
            recv_sem=stage_sem.at[1, item[0]],
            device_id={"rows": target[item[0]]},
            device_id_type=MESH,
        ).start()
    for p in late[1:]:
        sum_up(p)
    to_group(part, sum_sem)

    slots = {}
    for event, _ in schedule:
        if not isinstance(event, int):
            slots[event] = len(slots)

    def size_of(item):
        return depth if is_whole(item) and item not in ahead else half

    def whole(owner):
        return pl.ds(pl.multiple_of(owner * depth, half), depth)

    def part_of(owner, way):
        return pl.ds(pl.multiple_of(owner * depth + way * half, half), half)

    def held(item, sender):
        link, far, hop, _ = item
        if link == ACROSS:
            side_of = 0 if sender else 1
            owner = device(side_of, (0, -1, 1, 2, 2)[hop])
            return owner, None if hop < 3 else hop - 3
        away = hop - 1 if sender else hop
        return device(far, -away if link == UP else away), None if hop == 1 else link

    def rows_of(item, sender):
        owner, way = held(item, sender)
        if item in ahead:
            way = 1 - ahead[item]
        return whole(owner) if way is None else part_of(owner, way)

    def remote(item, sender):
        link, _, _, g = item
        ref = blocks[g].at[rows_of(item, sender), :]
        return pltpu.make_async_remote_copy(
            src_ref=ref,
            dst_ref=ref,
            send_sem=send_sem.at[link],
            recv_sem=recv_sem.at[slots[item]],
            device_id={"rows": target[link]},
            device_id_type=MESH,
        )

    sent = {}

    def send(item):
        remote(item, True).start()
        sent[item[0]] = sent.get(item[0], 0) + size_of(item) * len(pieces_of[item[3]])

    def share_with_twin(g, rows):
        ref = blocks[g].at[rows, :]
        pltpu.make_async_remote_copy(
            src_ref=ref,
            dst_ref=ref,
            send_sem=twin_sem.at[0, g // 2],
            recv_sem=twin_sem.at[1, g // 2],
            device_id={"rows": twin},
            device_id_type=MESH,
        ).start()

    def scales(ref, sems, size):
        drain(ref.at[pl.ds(0, n_rows - 1)], sems.at[1])
        total = ref[0, pl.ds(0, size), :]
        for d in range(1, n_rows):
            total = total + ref[d, pl.ds(0, size), :]
        scale = jnp.sqrt(total)
        return scale, 1.0 / scale

    early_scales = scales(early_part, early_sem, len(early))
    late_scales = None

    def take_in(item):
        link, _, _, g = item
        drain(stage.at[link], stage_sem.at[1, link])
        start = held(item, False)[0] * depth + ahead[item] * half
        by = late_scales[1][:1, :]

        def narrow(i, carry):
            rows = pl.ds(pl.multiple_of(i * step_rows, step_rows), step_rows)
            here = pl.ds(pl.multiple_of(start + i * step_rows, step_rows), step_rows)
            blocks[g][here, :] = (stage[link, rows, :] * by).astype(blocks[g].dtype)
            return carry

        lax.fori_loop(0, half // step_rows, narrow, 0)

    def make_block(g):
        pieces, out = pieces_of[g], blocks[g]
        scale, inverse = early_scales if pieces[0] in early else late_scales
        for p in pieces:
            _, _, col, at = groups[p]
            at_row = parts[p][1]
            col[pl.ds(at, wide)] = scale[at_row : at_row + 1, :].reshape(wide)

        def narrow(i, carry):
            rows = pl.ds(pl.multiple_of(i * tile, tile), tile)
            here = pl.ds(pl.multiple_of(me * depth + i * tile, tile), tile)
            for j, p in enumerate(pieces):
                at_row = parts[p][1]
                made = mixed[p, 0, rows, :] * inverse[at_row : at_row + 1, :]
                out[here, pl.ds(j * wide, wide)] = made.astype(out.dtype)
            return carry

        lax.fori_loop(0, depth // tile, narrow, 0)

    rows_half = n_rows // 2

    def meet():
        for d in range(n_rows):
            slab[lane, pl.ds(d % 2 * rows_half + d // 2, 1), :] = part[d, norm_at, :]
        for peer in along:
            pltpu.make_async_remote_copy(
                src_ref=slab.at[lane],
                dst_ref=slab.at[lane],
                send_sem=slab_sem.at[0, 0],
                recv_sem=slab_sem.at[0, 1],
                device_id={"width": peer},
                device_id_type=MESH,
            ).start()

    def swap():
        drain(slab.at[pl.ds(0, row - 1)], slab_sem.at[0, 1])
        mine = slab.at[pl.ds(lane // row * row, row)]
        pltpu.make_async_remote_copy(
            src_ref=mine,
            dst_ref=mine,
            send_sem=slab_sem.at[1, 0],
            recv_sem=slab_sem.at[1, 1],
            device_id={"width": opposite},
            device_id_type=MESH,
        ).start()

    def relay(way):
        return pltpu.make_async_remote_copy(
            src_ref=serve,
            dst_ref=serve,
            send_sem=relay_send.at[way],
            recv_sem=relay_recv.at[0],
            device_id={"rows": target.get(way, twin)},
            device_id_type=MESH,
        )

    def assemble():
        drain(slab.at[pl.ds(0, row)], slab_sem.at[1, 1])
        per_line = 2 * n_width * piece_size
        at_lane = lax.broadcasted_iota(jnp.int32, (rows_half, LANES), 1)
        tiles = [jnp.zeros((rows_half, LANES), jnp.float32)] * (per_line // LANES)
        for k in range(2 * n_width):
            x = slab[k % n_width, pl.ds(k // n_width * rows_half, rows_half), :]
            t, o = divmod(k * piece_size, LANES)
            x = pltpu.roll(x, o, 1) if o else x
            end = o + piece_size
            tiles[t] = jnp.where((at_lane >= o) & (at_lane < end), x, tiles[t])
            if end > LANES:
                tiles[t + 1] = jnp.where(at_lane < end - LANES, x, tiles[t + 1])
        for t, x in enumerate(tiles):
            for a in range(rows_half):
                flat[pl.ds(a * per_line + t * LANES, LANES)] = x[a : a + 1, :].reshape(LANES)
        serve[...] = flat[...].astype(serve.dtype)

    TWIN = 3
    lead = core == 0
    duties = [
        (envoy, (UP, DOWN, ACROSS, TWIN)),
        (lead & (place == 0) & (side == 1), (UP, DOWN, TWIN)),
        (lead & (place == 1), (UP, TWIN)),
        (lead & (place == 3), (TWIN,)),
        (lead & (place == 2), (TWIN,)),
        (core == 1, ()),
    ]

    def duty(i):
        role, ways = duties[i]

        @pl.when(role)
        def _():
            if i == 0:
                assemble()
            else:
                drain(serve, relay_recv.at[0])
            for way in ways:
                relay(way).start()

    moments = [len(schedule) * (3 + i) // 12 for i in range(len(duties))]
    meeting, swapping = len(blocks), (len(blocks) + moments[0]) // 2
    for index, (event, items) in enumerate(schedule):
        if index == meeting:
            pl.when(envoy)(meet)
        if index == swapping:
            pl.when(envoy)(swap)
        if index in moments:
            duty(moments.index(index))
        if isinstance(event, int):
            if late_scales is None and pieces_of[event][0] in late:
                late_scales = scales(part, sum_sem, len(late))
            make_block(event)
            g, rows = event, whole(me)
        else:
            if event in ahead:
                take_in(event)
            remote(event, False).wait_recv()
            g = event[3]
            rows = whole(held(event, False)[0]) if event in ahead else rows_of(event, False)
        for item in items:
            send(item)
        share_with_twin(g, rows)

    def drain_rows(rows, sem):
        drain(blocks[0].at[pl.ds(0, rows // len(pieces_of[0])), :], sem)

    for item in ahead:
        drain(stage.at[item[0]], stage_sem.at[0, item[0]])
    for link, rows in sent.items():
        drain_rows(rows, send_sem.at[link])
    for g in range(0, len(blocks), 2):
        for way in range(2):
            rows = depth * n_rows // 2 * sum(len(pieces) for pieces in pieces_of[g : g + 2])
            drain_rows(rows, twin_sem.at[way, g // 2])
    drain(early_part.at[pl.ds(0, n_rows - 1)], early_sem.at[0])
    drain(part.at[pl.ds(0, n_rows - 1)], sum_sem.at[0])
    for i, (role, ways) in enumerate(duties):

        @pl.when(role)
        def _(i=i, ways=ways):
            if i == 0:
                drain(slab.at[pl.ds(0, row - 1)], slab_sem.at[0, 0])
                drain(slab.at[pl.ds(0, row)], slab_sem.at[1, 0])
            for way in ways:
                relay(way).wait_send()


def store(pieces_of, wide, *refs):
    outs, sem = refs[-8:-1], refs[-1]
    blocks, small = refs[:-12], refs[-12:-8]
    pairs = list(zip(small, outs[3:]))
    for pieces, block in zip(pieces_of, blocks):
        lone = [p for p in pieces if p < 2]
        for j, p in enumerate(lone):
            pairs.append((block.at[:, pl.ds(j * wide, wide)], outs[1 + p]))
        if pieces[len(lone) :]:
            at, size = (pieces[len(lone)] - 2) * wide, (len(pieces) - len(lone)) * wide
            pairs.append((block.at[:, pl.ds(len(lone) * wide, size)], outs[0].at[:, pl.ds(at, size)]))
    copies = [pltpu.make_async_copy(src, dst, sem.at[i]) for i, (src, dst) in enumerate(pairs)]
    for copy in copies:
        copy.start()
    for copy in copies:
        copy.wait()


def solution(mesh):
    n_rows, n_width = mesh.shape["rows"], mesh.shape["width"]

    def shards(
        one_query,
        other_query,
        one_key,
        other_key,
        one_value,
        other_value,
        mix_share,
        norm_train,
        norm_step,
    ):
        depth, wide = one_key.shape
        wide_query = one_query.shape[1]
        count = 2 + wide_query // wide
        pieces_of, cross_first = layout(count)
        n_blocks = len(pieces_of)
        ahead = ahead_of(pieces_of, cross_first)
        schedule = plan([len(pieces) for pieces in pieces_of], cross_first, ahead)
        n_items = len(schedule) - n_blocks
        n_early = len(pieces_of[0]) + len(pieces_of[len(cross_first)])
        piece = norm_train.shape[0]
        total = depth * n_rows
        hbm = pl.BlockSpec(memory_space=pltpu.HBM)
        vmem = pl.BlockSpec(memory_space=pltpu.VMEM)
        dma = pltpu.SemaphoreType.DMA
        out_shape = tuple(
            pltpu.VMEM((total, wide * len(pieces)), jnp.bfloat16) for pieces in pieces_of
        ) + (
            pltpu.VMEM((wide_query,), jnp.float32),
            pltpu.VMEM((wide,), jnp.float32),
            pltpu.VMEM((wide,), jnp.float32),
            pltpu.VMEM((n_rows * n_width * piece,), jnp.bfloat16),
        )
        gathered = pl.pallas_call(
            lambda *refs: kernel(n_rows, n_width, pieces_of, cross_first, ahead, schedule, *refs),
            out_shape=out_shape,
            in_specs=[hbm] * 9,
            out_specs=[vmem] * (n_blocks + 4),
            scratch_shapes=[
                pltpu.VMEM((count, 2, depth, wide), jnp.float32),
                pltpu.VMEM((depth, LANES), jnp.float32),
                pltpu.VMEM((depth,), jnp.float32),
                pltpu.VMEM((piece,), jnp.float32),
                pltpu.VMEM((piece,), jnp.float32),
                pltpu.VMEM((n_rows, n_early, wide), jnp.float32),
                pltpu.VMEM((n_rows, count - n_early + 1, wide), jnp.float32),
                pltpu.VMEM((n_width, n_rows, LANES), jnp.float32),
                pltpu.VMEM((n_rows * n_width * piece,), jnp.float32),
                dma((count,)),
                dma((3,)),
                dma((2, 2)),
                dma((4,)),
                dma((1,)),
                dma((2,)),
                dma((2,)),
                dma((3,)),
                dma((n_items,)),
                dma((2, (n_blocks + 1) // 2)),
                pltpu.VMEM((3, depth // 2, wide), jnp.float32),
                dma((2, 3)),
            ],
            compiler_params=pltpu.CompilerParams(
                collective_id=0, has_side_effects=True, vmem_limit_bytes=44 * 1024 * 1024
            ),
        )(mix_share, norm_train, norm_step, one_query, other_query, one_key, other_key, one_value, other_value)
        return pl.pallas_call(
            lambda *refs: store(pieces_of, wide, *refs),
            out_shape=(
                jax.ShapeDtypeStruct((total, wide_query), jnp.bfloat16),
                jax.ShapeDtypeStruct((total, wide), jnp.bfloat16),
                jax.ShapeDtypeStruct((total, wide), jnp.bfloat16),
            )
            + tuple(jax.ShapeDtypeStruct(o.shape, o.dtype) for o in out_shape[n_blocks:]),
            in_specs=[vmem] * (n_blocks + 4),
            out_specs=[hbm] * 7,
            scratch_shapes=[dma((count + 4,))],
            compiler_params=pltpu.CompilerParams(vmem_limit_bytes=1024 * 1024),
        )(*gathered)

    wide_spec = P("rows", "width")
    in_specs = (wide_spec,) * 6 + (P("rows"), P(("rows", "width")), P(("rows", "width")))
    out_specs = (P(None, "width"),) * 3 + (P("width"),) * 3 + (P(),)
    return jax.shard_map(shards, mesh=mesh, in_specs=in_specs, out_specs=out_specs, check_vma=False)
```

```python
import jax
import jax.numpy as jnp
from jax import lax
from jax.experimental import pallas as pl
from jax.experimental.pallas import tpu as pltpu
from jax.sharding import PartitionSpec as P

MESH = pl.DeviceIdType.MESH
LANES = 128
CIRCLE = 4
UP, DOWN, ACROSS = 0, 1, 2
SPAN = 2
WINDOW = 4
DEPTH = 9
LAG = 0.7


def layout(count):
    first = (5 * count + 4) // 9

    def cut(start, end):
        return [list(range(i, min(i + SPAN, end))) for i in range(start, end, SPAN)]

    blocks = cut(0, first) + cut(first, count)
    return blocks, [b for b, pieces in enumerate(blocks) if pieces[0] < first]


def ahead_of(cross_first):
    last = cross_first[-1]
    return (UP, 0, 1, last), (DOWN, 0, 1, last), (ACROSS, 0, 0, last)


def plan(weights, cross_first, ahead, gone):
    free, flying, ready = [0.0] * 3, [0] * 3, [[], [], []]
    events, order, clock = [], [], [0]

    def put(now, event):
        clock[0] += 1
        events.append((now, clock[0], event))

    def offer(item):
        clock[0] += 1
        ready[item[0]].append((-steps_after(item, cross_first), clock[0], item))

    first = cross_first
    second = [b for b in range(len(weights)) if b not in cross_first]
    for k in range(max(len(first), len(second))):
        for b in second[k : k + 1] + first[k : k + 1]:
            put(0.1 * len(events), b)
    while events:
        events.sort()
        now, _, event = events.pop(0)
        if isinstance(event, int):
            for item in ((ACROSS, 0, 0, event), (UP, 0, 1, event), (DOWN, 0, 1, event)):
                offer(item)
        else:
            flying[event[0]] -= 1
            for item in followers(event, cross_first):
                offer(item)
        sends = []
        for link in (ACROSS, UP, DOWN):
            ready[link].sort()
            while ready[link] and flying[link] < DEPTH:
                item = ready[link].pop(0)[2]
                flying[link] += 1
                size = 1.0 - gone if item in ahead else 1.0 if is_whole(item) else 0.5
                free[link] = max(free[link], now) + size * weights[item[3]]
                put(free[link] + LAG, item)
                sends.append(item)
        order.append((event, sends))
    return order


def steps_after(item, cross_first):
    return max([1 + steps_after(x, cross_first) for x in followers(item, cross_first)], default=0)


def is_whole(item):
    link, _, hop, _ = item
    return hop < 3 if link == ACROSS else hop == 1


def followers(item, cross_first):
    link, far, hop, g = item
    if link == ACROSS:
        return [(UP, 1, 1, g), (DOWN, 1, 1, g)] if g in cross_first else []
    steps = [(link, far, 2, g)] if hop == 1 else []
    if g not in cross_first:
        steps.append((ACROSS, 0, 1 + link if hop == 1 else 3 + link, g))
    return steps


def kernel(
    n_rows,
    n_width,
    pieces_of,
    cross_first,
    ahead,
    schedule,
    share_in,
    norm_train,
    norm_step,
    one_query,
    other_query,
    one_key,
    other_key,
    one_value,
    other_value,
    *refs,
):
    blocks = refs[: len(pieces_of)]
    col_query, col_key, col_value, serve, mixed, share = refs[len(blocks) :][:6]
    line, train, step, early_part, part, slab, flat = refs[len(blocks) + 6 :][:7]
    in_sem, small_sem, slab_sem, relay_send, relay_recv = refs[len(blocks) + 13 :][:5]
    early_sem, sum_sem, send_sem, recv_sem, twin_sem = refs[len(blocks) + 18 :][:5]
    stage, stage_sem = refs[len(blocks) + 23 :]
    me = lax.axis_index("rows")
    lane = lax.axis_index("width")
    depth, wide = one_key.shape
    groups = [
        (one_key, other_key, col_key, 0),
        (one_value, other_value, col_value, 0),
    ] + [
        (one_query, other_query, col_query, j * wide)
        for j in range(one_query.shape[1] // wide)
    ]
    count = len(groups)
    tile = 64 if depth % 64 == 0 else 16
    half = depth // 2
    step_rows = 32

    def drain(ref, sem):
        pltpu.make_async_copy(ref, ref, sem).wait()

    small = []
    for i, (src, dst) in enumerate(((share_in, line), (norm_train, train), (norm_step, step))):
        small.append(pltpu.make_async_copy(src, dst, small_sem.at[i]))
        small[-1].start()

    early = pieces_of[len(cross_first)]
    (first_out,) = pieces_of[cross_first[-1]]
    late = [first_out] + [p for p in range(count) if p not in early + [first_out]]
    loading = early + late
    parts = {p: (early_part, k) for k, p in enumerate(early)}
    parts.update({p: (part, k) for k, p in enumerate(late)})

    def load(p):
        one, other, _, at = groups[p]
        for i, src in enumerate((one, other)):
            src = src.at[:, pl.ds(at, wide)]
            pltpu.make_async_copy(src, mixed.at[p, i], in_sem.at[p]).start()

    for p in loading[:WINDOW]:
        load(p)

    barrier = pltpu.get_barrier_semaphore()
    for d in range(1, n_rows):
        pl.semaphore_signal(
            barrier, inc=1, device_id={"rows": lax.rem(me + d, n_rows)}, device_id_type=MESH
        )

    envoy = me == 0
    row = n_width // 2
    along = [lane // row * row + (lane + d) % row for d in range(1, row)]
    opposite = (lane + row) % n_width

    @pl.when(envoy)
    def _():
        for peer in along + [opposite]:
            pl.semaphore_signal(barrier, inc=1, device_id={"width": peer}, device_id_type=MESH)

    for copy in small:
        copy.wait()
    piece_size = norm_train.shape[0]
    norm_at = pl.ds(len(late), 1)
    part[me, norm_at, :] = jnp.zeros((1, wide), jnp.float32)
    part[me, norm_at, pl.ds(0, piece_size)] = (train[...] + step[...]).reshape(1, -1)
    for at in range(0, depth, LANES):
        size = min(LANES, depth - at)
        piece = line[pl.ds(at, size)].reshape(1, size)
        share[pl.ds(at, size), :] = jnp.broadcast_to(piece, (LANES, size)).T

    core = me % 2
    place = (me // 2) % CIRCLE
    side = me // (2 * CIRCLE)

    def device(sides, steps, cores=0):
        chip = (side + sides) % 2 * CIRCLE + (place + steps + CIRCLE) % CIRCLE
        return chip * 2 + (core + cores) % 2

    far = [(a, b, c) for b in (2, 1, -1, 0) for a in (1, 0) for c in (1, 0) if (a, b, c) != (0, 0, 0)]

    def sum_up(p):
        drain(mixed.at[p], in_sem.at[p])
        if loading.index(p) + WINDOW < count:
            load(loading[loading.index(p) + WINDOW])

        def mix(i, acc):
            rows = pl.ds(pl.multiple_of(i * tile, tile), tile)
            s = share[rows, :]
            s = jnp.concatenate([s] * (wide // LANES), axis=1)
            r = s * mixed[p, 0, rows, :] + (1.0 - s) * mixed[p, 1, rows, :]
            mixed[p, 0, rows, :] = r
            return acc + jnp.sum((r * r).reshape(tile // 8, 8, wide), axis=0)

        acc = lax.fori_loop(0, depth // tile, mix, jnp.zeros((8, wide), jnp.float32))
        into, at_row = parts[p]
        into[me, pl.ds(at_row, 1), :] = jnp.sum(acc, axis=0, keepdims=True)

    def to_group(ref, sems):
        for where in far:
            pltpu.make_async_remote_copy(
                src_ref=ref.at[me],
                dst_ref=ref.at[me],
                send_sem=sems.at[0],
                recv_sem=sems.at[1],
                device_id={"rows": device(*where)},
                device_id_type=MESH,
            ).start()

    for p in early:
        sum_up(p)
    pl.semaphore_wait(barrier, n_rows - 1 + jnp.where(envoy, row, 0))
    to_group(early_part, early_sem)
    twin = me + 1 - 2 * core
    target = {UP: device(0, 1), DOWN: device(0, -1), ACROSS: device(1, 0)}
    sum_up(first_out)
    gone = stage.shape[1]
    for item in ahead:
        pltpu.make_async_remote_copy(
            src_ref=mixed.at[first_out, 0, pl.ds(0, gone), :],
            dst_ref=stage.at[item[0]],
            send_sem=stage_sem.at[0, item[0]],
            recv_sem=stage_sem.at[1, item[0]],
            device_id={"rows": target[item[0]]},
            device_id_type=MESH,
        ).start()
    for p in late[1:]:
        sum_up(p)
    to_group(part, sum_sem)

    slots = {}
    for event, _ in schedule:
        if not isinstance(event, int):
            slots[event] = len(slots)

    def size_of(item):
        return depth - gone if item in ahead else depth if is_whole(item) else half

    def whole(owner):
        return pl.ds(pl.multiple_of(owner * depth, half), depth)

    def part_of(owner, way):
        return pl.ds(pl.multiple_of(owner * depth + way * half, half), half)

    def held(item, sender):
        link, far, hop, _ = item
        if link == ACROSS:
            side_of = 0 if sender else 1
            owner = device(side_of, (0, -1, 1, 2, 2)[hop])
            return owner, None if hop < 3 else hop - 3
        away = hop - 1 if sender else hop
        return device(far, -away if link == UP else away), None if hop == 1 else link

    def rows_of(item, sender):
        owner, way = held(item, sender)
        if item in ahead:
            return pl.ds(pl.multiple_of(owner * depth + gone, 32), depth - gone)
        return whole(owner) if way is None else part_of(owner, way)

    def remote(item, sender):
        link, _, _, g = item
        ref = blocks[g].at[rows_of(item, sender), :]
        return pltpu.make_async_remote_copy(
            src_ref=ref,
            dst_ref=ref,
            send_sem=send_sem.at[link],
            recv_sem=recv_sem.at[slots[item]],
            device_id={"rows": target[link]},
            device_id_type=MESH,
        )

    sent = {}

    def send(item):
        remote(item, True).start()
        sent[item[0]] = sent.get(item[0], 0) + size_of(item) * len(pieces_of[item[3]])

    def share_with_twin(g, rows):
        ref = blocks[g].at[rows, :]
        pltpu.make_async_remote_copy(
            src_ref=ref,
            dst_ref=ref,
            send_sem=twin_sem.at[0, g // 2],
            recv_sem=twin_sem.at[1, g // 2],
            device_id={"rows": twin},
            device_id_type=MESH,
        ).start()

    def scales(ref, sems, size):
        drain(ref.at[pl.ds(0, n_rows - 1)], sems.at[1])
        total = ref[0, pl.ds(0, size), :]
        for d in range(1, n_rows):
            total = total + ref[d, pl.ds(0, size), :]
        scale = jnp.sqrt(total)
        return scale, 1.0 / scale

    early_scales = scales(early_part, early_sem, len(early))
    late_scales = None

    def take_in(item):
        link, _, _, g = item
        drain(stage.at[link], stage_sem.at[1, link])
        start = held(item, False)[0] * depth
        by = late_scales[1][:1, :]

        def narrow(i, carry):
            rows = pl.ds(pl.multiple_of(i * step_rows, step_rows), step_rows)
            here = pl.ds(pl.multiple_of(start + i * step_rows, step_rows), step_rows)
            blocks[g][here, :] = (stage[link, rows, :] * by).astype(blocks[g].dtype)
            return carry

        lax.fori_loop(0, gone // step_rows, narrow, 0)

    def make_block(g):
        pieces, out = pieces_of[g], blocks[g]
        scale, inverse = early_scales if pieces[0] in early else late_scales
        for p in pieces:
            _, _, col, at = groups[p]
            at_row = parts[p][1]
            col[pl.ds(at, wide)] = scale[at_row : at_row + 1, :].reshape(wide)

        def narrow(i, carry):
            rows = pl.ds(pl.multiple_of(i * tile, tile), tile)
            here = pl.ds(pl.multiple_of(me * depth + i * tile, tile), tile)
            for j, p in enumerate(pieces):
                at_row = parts[p][1]
                made = mixed[p, 0, rows, :] * inverse[at_row : at_row + 1, :]
                out[here, pl.ds(j * wide, wide)] = made.astype(out.dtype)
            return carry

        lax.fori_loop(0, depth // tile, narrow, 0)

    rows_half = n_rows // 2

    def meet():
        for d in range(n_rows):
            slab[lane, pl.ds(d % 2 * rows_half + d // 2, 1), :] = part[d, norm_at, :]
        for peer in along:
            pltpu.make_async_remote_copy(
                src_ref=slab.at[lane],
                dst_ref=slab.at[lane],
                send_sem=slab_sem.at[0, 0],
                recv_sem=slab_sem.at[0, 1],
                device_id={"width": peer},
                device_id_type=MESH,
            ).start()

    def swap():
        drain(slab.at[pl.ds(0, row - 1)], slab_sem.at[0, 1])
        mine = slab.at[pl.ds(lane // row * row, row)]
        pltpu.make_async_remote_copy(
            src_ref=mine,
            dst_ref=mine,
            send_sem=slab_sem.at[1, 0],
            recv_sem=slab_sem.at[1, 1],
            device_id={"width": opposite},
            device_id_type=MESH,
        ).start()

    def relay(way):
        return pltpu.make_async_remote_copy(
            src_ref=serve,
            dst_ref=serve,
            send_sem=relay_send.at[way],
            recv_sem=relay_recv.at[0],
            device_id={"rows": target.get(way, twin)},
            device_id_type=MESH,
        )

    def assemble():
        drain(slab.at[pl.ds(0, row)], slab_sem.at[1, 1])
        per_line = 2 * n_width * piece_size
        at_lane = lax.broadcasted_iota(jnp.int32, (rows_half, LANES), 1)
        tiles = [jnp.zeros((rows_half, LANES), jnp.float32)] * (per_line // LANES)
        for k in range(2 * n_width):
            x = slab[k % n_width, pl.ds(k // n_width * rows_half, rows_half), :]
            t, o = divmod(k * piece_size, LANES)
            x = pltpu.roll(x, o, 1) if o else x
            end = o + piece_size
            tiles[t] = jnp.where((at_lane >= o) & (at_lane < end), x, tiles[t])
            if end > LANES:
                tiles[t + 1] = jnp.where(at_lane < end - LANES, x, tiles[t + 1])
        for t, x in enumerate(tiles):
            for a in range(rows_half):
                flat[pl.ds(a * per_line + t * LANES, LANES)] = x[a : a + 1, :].reshape(LANES)
        serve[...] = flat[...].astype(serve.dtype)

    TWIN = 3
    lead = core == 0
    duties = [
        (envoy, (UP, DOWN, ACROSS, TWIN)),
        (lead & (place == 0) & (side == 1), (UP, DOWN, TWIN)),
        (lead & (place == 1), (UP, TWIN)),
        (lead & (place == 3), (TWIN,)),
        (lead & (place == 2), (TWIN,)),
        (core == 1, ()),
    ]

    def duty(i):
        role, ways = duties[i]

        @pl.when(role)
        def _():
            if i == 0:
                assemble()
            else:
                drain(serve, relay_recv.at[0])
            for way in ways:
                relay(way).start()

    moments = [len(schedule) * (3 + i) // 12 for i in range(len(duties))]
    meeting, swapping = len(blocks), (len(blocks) + moments[0]) // 2
    for index, (event, items) in enumerate(schedule):
        if index == meeting:
            pl.when(envoy)(meet)
        if index == swapping:
            pl.when(envoy)(swap)
        if index in moments:
            duty(moments.index(index))
        if isinstance(event, int):
            if late_scales is None and pieces_of[event][0] in late:
                late_scales = scales(part, sum_sem, len(late))
            make_block(event)
            g, rows = event, whole(me)
        else:
            if event in ahead:
                take_in(event)
            remote(event, False).wait_recv()
            g = event[3]
            rows = whole(held(event, False)[0]) if event in ahead else rows_of(event, False)
        for item in items:
            send(item)
        share_with_twin(g, rows)

    def drain_rows(rows, sem):
        drain(blocks[0].at[pl.ds(0, rows // len(pieces_of[0])), :], sem)

    for item in ahead:
        drain(stage.at[item[0]], stage_sem.at[0, item[0]])
    for link, rows in sent.items():
        drain_rows(rows, send_sem.at[link])
    for g in range(0, len(blocks), 2):
        for way in range(2):
            rows = depth * n_rows // 2 * sum(len(pieces) for pieces in pieces_of[g : g + 2])
            drain_rows(rows, twin_sem.at[way, g // 2])
    drain(early_part.at[pl.ds(0, n_rows - 1)], early_sem.at[0])
    drain(part.at[pl.ds(0, n_rows - 1)], sum_sem.at[0])
    for i, (role, ways) in enumerate(duties):

        @pl.when(role)
        def _(i=i, ways=ways):
            if i == 0:
                drain(slab.at[pl.ds(0, row - 1)], slab_sem.at[0, 0])
                drain(slab.at[pl.ds(0, row)], slab_sem.at[1, 0])
            for way in ways:
                relay(way).wait_send()


def store(pieces_of, wide, *refs):
    outs, sem = refs[-8:-1], refs[-1]
    blocks, small = refs[:-12], refs[-12:-8]
    pairs = list(zip(small, outs[3:]))
    for pieces, block in zip(pieces_of, blocks):
        lone = [p for p in pieces if p < 2]
        for j, p in enumerate(lone):
            pairs.append((block.at[:, pl.ds(j * wide, wide)], outs[1 + p]))
        if pieces[len(lone) :]:
            at, size = (pieces[len(lone)] - 2) * wide, (len(pieces) - len(lone)) * wide
            pairs.append((block.at[:, pl.ds(len(lone) * wide, size)], outs[0].at[:, pl.ds(at, size)]))
    copies = [pltpu.make_async_copy(src, dst, sem.at[i]) for i, (src, dst) in enumerate(pairs)]
    for copy in copies:
        copy.start()
    for copy in copies:
        copy.wait()


def solution(mesh):
    n_rows, n_width = mesh.shape["rows"], mesh.shape["width"]

    def shards(
        one_query,
        other_query,
        one_key,
        other_key,
        one_value,
        other_value,
        mix_share,
        norm_train,
        norm_step,
    ):
        depth, wide = one_key.shape
        wide_query = one_query.shape[1]
        count = 2 + wide_query // wide
        pieces_of, cross_first = layout(count)
        n_blocks = len(pieces_of)
        ahead = ahead_of(cross_first)
        gone = depth * 5 // 7 // 32 * 32
        schedule = plan([len(pieces) for pieces in pieces_of], cross_first, ahead, gone / depth)
        n_items = len(schedule) - n_blocks
        n_early = len(pieces_of[len(cross_first)])
        piece = norm_train.shape[0]
        total = depth * n_rows
        hbm = pl.BlockSpec(memory_space=pltpu.HBM)
        vmem = pl.BlockSpec(memory_space=pltpu.VMEM)
        dma = pltpu.SemaphoreType.DMA
        out_shape = tuple(
            pltpu.VMEM((total, wide * len(pieces)), jnp.bfloat16) for pieces in pieces_of
        ) + (
            pltpu.VMEM((wide_query,), jnp.float32),
            pltpu.VMEM((wide,), jnp.float32),
            pltpu.VMEM((wide,), jnp.float32),
            pltpu.VMEM((n_rows * n_width * piece,), jnp.bfloat16),
        )
        gathered = pl.pallas_call(
            lambda *refs: kernel(n_rows, n_width, pieces_of, cross_first, ahead, schedule, *refs),
            out_shape=out_shape,
            in_specs=[hbm] * 9,
            out_specs=[vmem] * (n_blocks + 4),
            scratch_shapes=[
                pltpu.VMEM((count, 2, depth, wide), jnp.float32),
                pltpu.VMEM((depth, LANES), jnp.float32),
                pltpu.VMEM((depth,), jnp.float32),
                pltpu.VMEM((piece,), jnp.float32),
                pltpu.VMEM((piece,), jnp.float32),
                pltpu.VMEM((n_rows, n_early, wide), jnp.float32),
                pltpu.VMEM((n_rows, count - n_early + 1, wide), jnp.float32),
                pltpu.VMEM((n_width, n_rows, LANES), jnp.float32),
                pltpu.VMEM((n_rows * n_width * piece,), jnp.float32),
                dma((count,)),
                dma((3,)),
                dma((2, 2)),
                dma((4,)),
                dma((1,)),
                dma((2,)),
                dma((2,)),
                dma((3,)),
                dma((n_items,)),
                dma((2, (n_blocks + 1) // 2)),
                pltpu.VMEM((3, gone, wide), jnp.float32),
                dma((2, 3)),
            ],
            compiler_params=pltpu.CompilerParams(
                collective_id=0, has_side_effects=True, vmem_limit_bytes=44 * 1024 * 1024
            ),
        )(mix_share, norm_train, norm_step, one_query, other_query, one_key, other_key, one_value, other_value)
        return pl.pallas_call(
            lambda *refs: store(pieces_of, wide, *refs),
            out_shape=(
                jax.ShapeDtypeStruct((total, wide_query), jnp.bfloat16),
                jax.ShapeDtypeStruct((total, wide), jnp.bfloat16),
                jax.ShapeDtypeStruct((total, wide), jnp.bfloat16),
            )
            + tuple(jax.ShapeDtypeStruct(o.shape, o.dtype) for o in out_shape[n_blocks:]),
            in_specs=[vmem] * (n_blocks + 4),
            out_specs=[hbm] * 7,
            scratch_shapes=[dma((count + 4,))],
            compiler_params=pltpu.CompilerParams(vmem_limit_bytes=1024 * 1024),
        )(*gathered)

    wide_spec = P("rows", "width")
    in_specs = (wide_spec,) * 6 + (P("rows"), P(("rows", "width")), P(("rows", "width")))
    out_specs = (P(None, "width"),) * 3 + (P("width"),) * 3 + (P(),)
    return jax.shard_map(shards, mesh=mesh, in_specs=in_specs, out_specs=out_specs, check_vma=False)
```

```python
import jax
import jax.numpy as jnp
from jax import lax
from jax.experimental import pallas as pl
from jax.experimental.pallas import tpu as pltpu
from jax.sharding import PartitionSpec as P

MESH = pl.DeviceIdType.MESH
LANES = 128
CIRCLE = 4
UP, DOWN, ACROSS = 0, 1, 2
SPAN = 2
WINDOW = 4
DEPTH = 9
LAG = 0.7


def layout(count):
    first = (5 * count + 4) // 9

    def cut(start, end):
        return [list(range(i, min(i + SPAN, end))) for i in range(start, end, SPAN)]

    blocks = cut(0, first) + cut(first, count)
    return blocks, [b for b, pieces in enumerate(blocks) if pieces[0] < first]


def ahead_of(cross_first):
    last = cross_first[-1]
    return (UP, 0, 1, last), (DOWN, 0, 1, last), (ACROSS, 0, 0, last)


def plan(weights, cross_first, ahead, gone):
    free, flying, ready = [0.0] * 3, [0] * 3, [[], [], []]
    events, order, clock = [], [], [0]

    def put(now, event):
        clock[0] += 1
        events.append((now, clock[0], event))

    def offer(item):
        clock[0] += 1
        ready[item[0]].append((-steps_after(item, cross_first), clock[0], item))

    first = cross_first
    second = [b for b in range(len(weights)) if b not in cross_first]
    for k in range(max(len(first), len(second))):
        for b in first[k : k + 1] + second[k : k + 1]:
            put(0.1 * len(events), b)
    while events:
        events.sort()
        now, _, event = events.pop(0)
        if isinstance(event, int):
            for item in ((ACROSS, 0, 0, event), (UP, 0, 1, event), (DOWN, 0, 1, event)):
                offer(item)
        else:
            flying[event[0]] -= 1
            for item in followers(event, cross_first):
                offer(item)
        sends = []
        for link in (ACROSS, UP, DOWN):
            ready[link].sort()
            while ready[link] and flying[link] < DEPTH:
                item = ready[link].pop(0)[2]
                flying[link] += 1
                size = 1.0 - gone if item in ahead else 1.0 if is_whole(item) else 0.5
                free[link] = max(free[link], now) + size * weights[item[3]]
                put(free[link] + LAG, item)
                sends.append(item)
        order.append((event, sends))
    return order


def arrival(item, cross_first):
    link, far, hop, block = item
    together = link != ACROSS and hop == 2 and block in cross_first
    return (UP, far, hop, block) if together else item


def steps_after(item, cross_first):
    return max([1 + steps_after(x, cross_first) for x in followers(item, cross_first)], default=0)


def is_whole(item):
    link, _, hop, _ = item
    return hop < 3 if link == ACROSS else hop == 1


def followers(item, cross_first):
    link, far, hop, g = item
    if link == ACROSS:
        return [(UP, 1, 1, g), (DOWN, 1, 1, g)] if g in cross_first else []
    steps = [(link, far, 2, g)] if hop == 1 else []
    if g not in cross_first:
        steps.append((ACROSS, 0, 1 + link if hop == 1 else 3 + link, g))
    return steps


def kernel(
    n_rows,
    n_width,
    pieces_of,
    cross_first,
    ahead,
    schedule,
    share_in,
    norm_train,
    norm_step,
    one_query,
    other_query,
    one_key,
    other_key,
    one_value,
    other_value,
    *refs,
):
    blocks = refs[: len(pieces_of)]
    col_query, col_key, col_value, serve, mixed, share = refs[len(blocks) :][:6]
    line, train, step, early_part, part, slab, flat = refs[len(blocks) + 6 :][:7]
    in_sem, small_sem, slab_sem, relay_send, relay_recv = refs[len(blocks) + 13 :][:5]
    early_sem, sum_sem, send_sem, recv_sem, twin_sem = refs[len(blocks) + 18 :][:5]
    stage, stage_sem = refs[len(blocks) + 23 :]
    me = lax.axis_index("rows")
    lane = lax.axis_index("width")
    depth, wide = one_key.shape
    groups = [
        (one_key, other_key, col_key, 0),
        (one_value, other_value, col_value, 0),
    ] + [
        (one_query, other_query, col_query, j * wide)
        for j in range(one_query.shape[1] // wide)
    ]
    count = len(groups)
    tile = 64 if depth % 64 == 0 else 16
    half = depth // 2
    step_rows = 32

    def drain(ref, sem):
        pltpu.make_async_copy(ref, ref, sem).wait()

    small = []
    for i, (src, dst) in enumerate(((share_in, line), (norm_train, train), (norm_step, step))):
        small.append(pltpu.make_async_copy(src, dst, small_sem.at[i]))
        small[-1].start()

    early = pieces_of[0]
    (first_out,) = pieces_of[cross_first[-1]]
    late = [first_out] + [p for p in range(count) if p not in early + [first_out]]
    loading = early + late
    parts = {p: (early_part, k) for k, p in enumerate(early)}
    parts.update({p: (part, k) for k, p in enumerate(late)})

    def load(p):
        one, other, _, at = groups[p]
        for i, src in enumerate((one, other)):
            src = src.at[:, pl.ds(at, wide)]
            pltpu.make_async_copy(src, mixed.at[p, i], in_sem.at[p]).start()

    for p in loading[:WINDOW]:
        load(p)

    barrier = pltpu.get_barrier_semaphore()
    for d in range(1, n_rows):
        pl.semaphore_signal(
            barrier, inc=1, device_id={"rows": lax.rem(me + d, n_rows)}, device_id_type=MESH
        )

    envoy = me == 0
    row = n_width // 2
    along = [lane // row * row + (lane + d) % row for d in range(1, row)]
    opposite = (lane + row) % n_width

    @pl.when(envoy)
    def _():
        for peer in along + [opposite]:
            pl.semaphore_signal(barrier, inc=1, device_id={"width": peer}, device_id_type=MESH)

    for copy in small:
        copy.wait()
    piece_size = norm_train.shape[0]
    norm_at = pl.ds(len(late), 1)
    part[me, norm_at, :] = jnp.zeros((1, wide), jnp.float32)
    part[me, norm_at, pl.ds(0, piece_size)] = (train[...] + step[...]).reshape(1, -1)
    for at in range(0, depth, LANES):
        size = min(LANES, depth - at)
        piece = line[pl.ds(at, size)].reshape(1, size)
        share[pl.ds(at, size), :] = jnp.broadcast_to(piece, (LANES, size)).T

    core = me % 2
    place = (me // 2) % CIRCLE
    side = me // (2 * CIRCLE)

    def device(sides, steps, cores=0):
        chip = (side + sides) % 2 * CIRCLE + (place + steps + CIRCLE) % CIRCLE
        return chip * 2 + (core + cores) % 2

    far = [(a, b, c) for b in (2, 1, -1, 0) for a in (1, 0) for c in (1, 0) if (a, b, c) != (0, 0, 0)]

    def sum_up(p):
        drain(mixed.at[p], in_sem.at[p])
        if loading.index(p) + WINDOW < count:
            load(loading[loading.index(p) + WINDOW])

        def mix(i, acc):
            rows = pl.ds(pl.multiple_of(i * tile, tile), tile)
            s = share[rows, :]
            s = jnp.concatenate([s] * (wide // LANES), axis=1)
            r = s * mixed[p, 0, rows, :] + (1.0 - s) * mixed[p, 1, rows, :]
            mixed[p, 0, rows, :] = r
            return acc + jnp.sum((r * r).reshape(tile // 8, 8, wide), axis=0)

        acc = lax.fori_loop(0, depth // tile, mix, jnp.zeros((8, wide), jnp.float32))
        into, at_row = parts[p]
        into[me, pl.ds(at_row, 1), :] = jnp.sum(acc, axis=0, keepdims=True)

    def to_group(ref, sems):
        for where in far:
            pltpu.make_async_remote_copy(
                src_ref=ref.at[me],
                dst_ref=ref.at[me],
                send_sem=sems.at[0],
                recv_sem=sems.at[1],
                device_id={"rows": device(*where)},
                device_id_type=MESH,
            ).start()

    for p in early:
        sum_up(p)
    pl.semaphore_wait(barrier, n_rows - 1 + jnp.where(envoy, row, 0))
    to_group(early_part, early_sem)
    twin = me + 1 - 2 * core
    target = {UP: device(0, 1), DOWN: device(0, -1), ACROSS: device(1, 0)}
    sum_up(first_out)
    gone = stage.shape[1]
    for item in ahead:
        pltpu.make_async_remote_copy(
            src_ref=mixed.at[first_out, 0, pl.ds(0, gone), :],
            dst_ref=stage.at[item[0]],
            send_sem=stage_sem.at[0, item[0]],
            recv_sem=stage_sem.at[1, item[0]],
            device_id={"rows": target[item[0]]},
            device_id_type=MESH,
        ).start()
    for p in late[1:]:
        sum_up(p)
    to_group(part, sum_sem)

    slots = {}
    for event, _ in schedule:
        if not isinstance(event, int):
            slots.setdefault(arrival(event, cross_first), len(slots))

    def size_of(item):
        return depth - gone if item in ahead else depth if is_whole(item) else half

    def whole(owner):
        return pl.ds(pl.multiple_of(owner * depth, half), depth)

    def part_of(owner, way):
        return pl.ds(pl.multiple_of(owner * depth + way * half, half), half)

    def held(item, sender):
        link, far, hop, _ = item
        if link == ACROSS:
            side_of = 0 if sender else 1
            owner = device(side_of, (0, -1, 1, 2, 2)[hop])
            return owner, None if hop < 3 else hop - 3
        away = hop - 1 if sender else hop
        return device(far, -away if link == UP else away), None if hop == 1 else link

    def rows_of(item, sender):
        owner, way = held(item, sender)
        if item in ahead:
            return pl.ds(pl.multiple_of(owner * depth + gone, 32), depth - gone)
        return whole(owner) if way is None else part_of(owner, way)

    def remote(item, sender):
        link, _, _, g = item
        ref = blocks[g].at[rows_of(item, sender), :]
        return pltpu.make_async_remote_copy(
            src_ref=ref,
            dst_ref=ref,
            send_sem=send_sem.at[link],
            recv_sem=recv_sem.at[slots[arrival(item, cross_first)]],
            device_id={"rows": target[link]},
            device_id_type=MESH,
        )

    sent = {}

    def send(item):
        remote(item, True).start()
        sent[item[0]] = sent.get(item[0], 0) + size_of(item) * len(pieces_of[item[3]])

    def share_with_twin(g, rows):
        ref = blocks[g].at[rows, :]
        pltpu.make_async_remote_copy(
            src_ref=ref,
            dst_ref=ref,
            send_sem=twin_sem.at[0, g // 2],
            recv_sem=twin_sem.at[1, g // 2],
            device_id={"rows": twin},
            device_id_type=MESH,
        ).start()

    def scales(ref, sems, size):
        drain(ref.at[pl.ds(0, n_rows - 1)], sems.at[1])
        total = ref[0, pl.ds(0, size), :]
        for d in range(1, n_rows):
            total = total + ref[d, pl.ds(0, size), :]
        scale = jnp.sqrt(total)
        return scale, 1.0 / scale

    early_scales = scales(early_part, early_sem, len(early))
    late_scales = None

    def take_in(item):
        link, _, _, g = item
        drain(stage.at[link], stage_sem.at[1, link])
        start = held(item, False)[0] * depth
        by = late_scales[1][:1, :]

        def narrow(i, carry):
            rows = pl.ds(pl.multiple_of(i * step_rows, step_rows), step_rows)
            here = pl.ds(pl.multiple_of(start + i * step_rows, step_rows), step_rows)
            blocks[g][here, :] = (stage[link, rows, :] * by).astype(blocks[g].dtype)
            return carry

        lax.fori_loop(0, gone // step_rows, narrow, 0)

    def make_block(g):
        pieces, out = pieces_of[g], blocks[g]
        scale, inverse = early_scales if pieces[0] in early else late_scales
        for p in pieces:
            _, _, col, at = groups[p]
            at_row = parts[p][1]
            col[pl.ds(at, wide)] = scale[at_row : at_row + 1, :].reshape(wide)

        def narrow(i, carry):
            rows = pl.ds(pl.multiple_of(i * tile, tile), tile)
            here = pl.ds(pl.multiple_of(me * depth + i * tile, tile), tile)
            for j, p in enumerate(pieces):
                at_row = parts[p][1]
                made = mixed[p, 0, rows, :] * inverse[at_row : at_row + 1, :]
                out[here, pl.ds(j * wide, wide)] = made.astype(out.dtype)
            return carry

        lax.fori_loop(0, depth // tile, narrow, 0)

    rows_half = n_rows // 2

    def meet():
        for d in range(n_rows):
            slab[lane, pl.ds(d % 2 * rows_half + d // 2, 1), :] = part[d, norm_at, :]
        for peer in along:
            pltpu.make_async_remote_copy(
                src_ref=slab.at[lane],
                dst_ref=slab.at[lane],
                send_sem=slab_sem.at[0, 0],
                recv_sem=slab_sem.at[0, 1],
                device_id={"width": peer},
                device_id_type=MESH,
            ).start()

    def swap():
        drain(slab.at[pl.ds(0, row - 1)], slab_sem.at[0, 1])
        mine = slab.at[pl.ds(lane // row * row, row)]
        pltpu.make_async_remote_copy(
            src_ref=mine,
            dst_ref=mine,
            send_sem=slab_sem.at[1, 0],
            recv_sem=slab_sem.at[1, 1],
            device_id={"width": opposite},
            device_id_type=MESH,
        ).start()

    def relay(way):
        return pltpu.make_async_remote_copy(
            src_ref=serve,
            dst_ref=serve,
            send_sem=relay_send.at[way],
            recv_sem=relay_recv.at[0],
            device_id={"rows": target.get(way, twin)},
            device_id_type=MESH,
        )

    def assemble():
        drain(slab.at[pl.ds(0, row)], slab_sem.at[1, 1])
        per_line = 2 * n_width * piece_size
        at_lane = lax.broadcasted_iota(jnp.int32, (rows_half, LANES), 1)
        tiles = [jnp.zeros((rows_half, LANES), jnp.float32)] * (per_line // LANES)
        for k in range(2 * n_width):
            x = slab[k % n_width, pl.ds(k // n_width * rows_half, rows_half), :]
            t, o = divmod(k * piece_size, LANES)
            x = pltpu.roll(x, o, 1) if o else x
            end = o + piece_size
            tiles[t] = jnp.where((at_lane >= o) & (at_lane < end), x, tiles[t])
            if end > LANES:
                tiles[t + 1] = jnp.where(at_lane < end - LANES, x, tiles[t + 1])
        for t, x in enumerate(tiles):
            for a in range(rows_half):
                flat[pl.ds(a * per_line + t * LANES, LANES)] = x[a : a + 1, :].reshape(LANES)
        serve[...] = flat[...].astype(serve.dtype)

    TWIN = 3
    lead = core == 0
    duties = [
        (envoy, (UP, DOWN, ACROSS, TWIN)),
        (lead & (place == 0) & (side == 1), (UP, DOWN, TWIN)),
        (lead & (place == 1), (UP, TWIN)),
        (lead & (place == 3), (TWIN,)),
        (lead & (place == 2), (TWIN,)),
        (core == 1, ()),
    ]

    def duty(i):
        role, ways = duties[i]

        @pl.when(role)
        def _():
            if i == 0:
                assemble()
            else:
                drain(serve, relay_recv.at[0])
            for way in ways:
                relay(way).start()

    moments = [len(schedule) * (3 + i) // 12 for i in range(len(duties))]
    halves = set()
    meeting, swapping = len(blocks), (len(blocks) + moments[0]) // 2
    for index, (event, items) in enumerate(schedule):
        if index == meeting:
            pl.when(envoy)(meet)
        if index == swapping:
            pl.when(envoy)(swap)
        if index in moments:
            duty(moments.index(index))
        if isinstance(event, int):
            if late_scales is None and pieces_of[event][0] in late:
                late_scales = scales(part, sum_sem, len(late))
            make_block(event)
            g, rows = event, whole(me)
        else:
            if event in ahead:
                take_in(event)
            g, rows = event[3], rows_of(event, False)
            known = arrival(event, cross_first)
            if is_whole(event) or g not in cross_first:
                remote(event, False).wait_recv()
            elif known in halves:
                rows = whole(held(event, False)[0])
                drain(blocks[g].at[rows, :], recv_sem.at[slots[known]])
            else:
                halves.add(known)
                rows = None
            if event in ahead:
                rows = whole(held(event, False)[0])
        for item in items:
            send(item)
        if rows is not None:
            share_with_twin(g, rows)

    def drain_rows(rows, sem):
        drain(blocks[0].at[pl.ds(0, rows // len(pieces_of[0])), :], sem)

    for item in ahead:
        drain(stage.at[item[0]], stage_sem.at[0, item[0]])
    for link, rows in sent.items():
        drain_rows(rows, send_sem.at[link])
    for g in range(0, len(blocks), 2):
        for way in range(2):
            rows = depth * n_rows // 2 * sum(len(pieces) for pieces in pieces_of[g : g + 2])
            drain_rows(rows, twin_sem.at[way, g // 2])
    drain(early_part.at[pl.ds(0, n_rows - 1)], early_sem.at[0])
    drain(part.at[pl.ds(0, n_rows - 1)], sum_sem.at[0])
    for i, (role, ways) in enumerate(duties):

        @pl.when(role)
        def _(i=i, ways=ways):
            if i == 0:
                drain(slab.at[pl.ds(0, row - 1)], slab_sem.at[0, 0])
                drain(slab.at[pl.ds(0, row)], slab_sem.at[1, 0])
            for way in ways:
                relay(way).wait_send()


def store(pieces_of, wide, *refs):
    outs, sem = refs[-8:-1], refs[-1]
    blocks, small = refs[:-12], refs[-12:-8]
    pairs = list(zip(small, outs[3:]))
    for pieces, block in zip(pieces_of, blocks):
        lone = [p for p in pieces if p < 2]
        for j, p in enumerate(lone):
            pairs.append((block.at[:, pl.ds(j * wide, wide)], outs[1 + p]))
        if pieces[len(lone) :]:
            at, size = (pieces[len(lone)] - 2) * wide, (len(pieces) - len(lone)) * wide
            pairs.append((block.at[:, pl.ds(len(lone) * wide, size)], outs[0].at[:, pl.ds(at, size)]))
    copies = [pltpu.make_async_copy(src, dst, sem.at[i]) for i, (src, dst) in enumerate(pairs)]
    for copy in copies:
        copy.start()
    for copy in copies:
        copy.wait()


def solution(mesh):
    n_rows, n_width = mesh.shape["rows"], mesh.shape["width"]

    def shards(
        one_query,
        other_query,
        one_key,
        other_key,
        one_value,
        other_value,
        mix_share,
        norm_train,
        norm_step,
    ):
        depth, wide = one_key.shape
        wide_query = one_query.shape[1]
        count = 2 + wide_query // wide
        pieces_of, cross_first = layout(count)
        n_blocks = len(pieces_of)
        ahead = ahead_of(cross_first)
        gone = depth * 5 // 7 // 32 * 32
        schedule = plan([len(pieces) for pieces in pieces_of], cross_first, ahead, gone / depth)
        n_items = len({arrival(e, cross_first) for e, _ in schedule if not isinstance(e, int)})
        n_early = len(pieces_of[0])
        piece = norm_train.shape[0]
        total = depth * n_rows
        hbm = pl.BlockSpec(memory_space=pltpu.HBM)
        vmem = pl.BlockSpec(memory_space=pltpu.VMEM)
        dma = pltpu.SemaphoreType.DMA
        out_shape = tuple(
            pltpu.VMEM((total, wide * len(pieces)), jnp.bfloat16) for pieces in pieces_of
        ) + (
            pltpu.VMEM((wide_query,), jnp.float32),
            pltpu.VMEM((wide,), jnp.float32),
            pltpu.VMEM((wide,), jnp.float32),
            pltpu.VMEM((n_rows * n_width * piece,), jnp.bfloat16),
        )
        gathered = pl.pallas_call(
            lambda *refs: kernel(n_rows, n_width, pieces_of, cross_first, ahead, schedule, *refs),
            out_shape=out_shape,
            in_specs=[hbm] * 9,
            out_specs=[vmem] * (n_blocks + 4),
            scratch_shapes=[
                pltpu.VMEM((count, 2, depth, wide), jnp.float32),
                pltpu.VMEM((depth, LANES), jnp.float32),
                pltpu.VMEM((depth,), jnp.float32),
                pltpu.VMEM((piece,), jnp.float32),
                pltpu.VMEM((piece,), jnp.float32),
                pltpu.VMEM((n_rows, n_early, wide), jnp.float32),
                pltpu.VMEM((n_rows, count - n_early + 1, wide), jnp.float32),
                pltpu.VMEM((n_width, n_rows, LANES), jnp.float32),
                pltpu.VMEM((n_rows * n_width * piece,), jnp.float32),
                dma((count,)),
                dma((3,)),
                dma((2, 2)),
                dma((4,)),
                dma((1,)),
                dma((2,)),
                dma((2,)),
                dma((3,)),
                dma((n_items,)),
                dma((2, (n_blocks + 1) // 2)),
                pltpu.VMEM((3, gone, wide), jnp.float32),
                dma((2, 3)),
            ],
            compiler_params=pltpu.CompilerParams(
                collective_id=0, has_side_effects=True, vmem_limit_bytes=44 * 1024 * 1024
            ),
        )(mix_share, norm_train, norm_step, one_query, other_query, one_key, other_key, one_value, other_value)
        return pl.pallas_call(
            lambda *refs: store(pieces_of, wide, *refs),
            out_shape=(
                jax.ShapeDtypeStruct((total, wide_query), jnp.bfloat16),
                jax.ShapeDtypeStruct((total, wide), jnp.bfloat16),
                jax.ShapeDtypeStruct((total, wide), jnp.bfloat16),
            )
            + tuple(jax.ShapeDtypeStruct(o.shape, o.dtype) for o in out_shape[n_blocks:]),
            in_specs=[vmem] * (n_blocks + 4),
            out_specs=[hbm] * 7,
            scratch_shapes=[dma((n_blocks + 5,))],
            compiler_params=pltpu.CompilerParams(vmem_limit_bytes=1024 * 1024),
        )(*gathered)

    wide_spec = P("rows", "width")
    in_specs = (wide_spec,) * 6 + (P("rows"), P(("rows", "width")), P(("rows", "width")))
    out_specs = (P(None, "width"),) * 3 + (P("width"),) * 3 + (P(),)
    return jax.shard_map(shards, mesh=mesh, in_specs=in_specs, out_specs=out_specs, check_vma=False)
```

```python
import jax
import jax.numpy as jnp
from jax import lax
from jax.experimental import pallas as pl
from jax.experimental.pallas import tpu as pltpu
from jax.sharding import PartitionSpec as P

MESH = pl.DeviceIdType.MESH
LANES = 128
CIRCLE = 4
UP, DOWN, ACROSS = 0, 1, 2
SPAN = 2
WINDOW = 4
DEPTH = 9
LAG = 0.7


def layout(count):
    first = (5 * count + 4) // 9

    def cut(start, end):
        return [list(range(i, min(i + SPAN, end))) for i in range(start, end, SPAN)]

    blocks = cut(0, first) + cut(first, count)
    return blocks, [b for b, pieces in enumerate(blocks) if pieces[0] < first]


def ahead_of(cross_first):
    last = cross_first[-1]
    return (UP, 0, 1, last), (DOWN, 0, 1, last), (ACROSS, 0, 0, last)


def plan(weights, cross_first, ahead, gone):
    free, flying, ready = [0.0] * 3, [0] * 3, [[], [], []]
    events, order, clock = [], [], [0]

    def put(now, event):
        clock[0] += 1
        events.append((now, clock[0], event))

    def offer(item):
        clock[0] += 1
        ready[item[0]].append((-steps_after(item, cross_first), clock[0], item))

    first = cross_first
    second = [b for b in range(len(weights)) if b not in cross_first]
    for k in range(max(len(first), len(second))):
        for b in second[k : k + 1] + first[k : k + 1]:
            put(0.1 * len(events), b)
    while events:
        events.sort()
        now, _, event = events.pop(0)
        if isinstance(event, int):
            for item in ((ACROSS, 0, 0, event), (UP, 0, 1, event), (DOWN, 0, 1, event)):
                offer(item)
        else:
            flying[event[0]] -= 1
            for item in followers(event, cross_first):
                offer(item)
        sends = []
        for link in (ACROSS, UP, DOWN):
            ready[link].sort()
            while ready[link] and flying[link] < DEPTH:
                item = ready[link].pop(0)[2]
                flying[link] += 1
                size = 1.0 - gone if item in ahead else 1.0 if is_whole(item) else 0.5
                free[link] = max(free[link], now) + size * weights[item[3]]
                put(free[link] + LAG, item)
                sends.append(item)
        order.append((event, sends))
    return order


def steps_after(item, cross_first):
    return max([1 + steps_after(x, cross_first) for x in followers(item, cross_first)], default=0)


def is_whole(item):
    link, _, hop, _ = item
    return hop < 3 if link == ACROSS else hop == 1


def followers(item, cross_first):
    link, far, hop, g = item
    if link == ACROSS:
        return [(UP, 1, 1, g), (DOWN, 1, 1, g)] if g in cross_first else []
    steps = [(link, far, 2, g)] if hop == 1 else []
    if g not in cross_first:
        steps.append((ACROSS, 0, 1 + link if hop == 1 else 3 + link, g))
    return steps


def kernel(
    n_rows,
    n_width,
    pieces_of,
    cross_first,
    ahead,
    schedule,
    share_in,
    norm_train,
    norm_step,
    one_query,
    other_query,
    one_key,
    other_key,
    one_value,
    other_value,
    *refs,
):
    blocks = refs[: len(pieces_of)]
    col_query, col_key, col_value, serve, mixed, share = refs[len(blocks) :][:6]
    line, train, step, early_part, part, slab, flat = refs[len(blocks) + 6 :][:7]
    in_sem, small_sem, slab_sem, relay_send, relay_recv = refs[len(blocks) + 13 :][:5]
    early_sem, sum_sem, send_sem, recv_sem, twin_sem = refs[len(blocks) + 18 :][:5]
    stage, stage_sem = refs[len(blocks) + 23 :]
    me = lax.axis_index("rows")
    lane = lax.axis_index("width")
    depth, wide = one_key.shape
    groups = [
        (one_key, other_key, col_key, 0),
        (one_value, other_value, col_value, 0),
    ] + [
        (one_query, other_query, col_query, j * wide)
        for j in range(one_query.shape[1] // wide)
    ]
    count = len(groups)
    tile = 64 if depth % 64 == 0 else 16
    half = depth // 2
    step_rows = 32

    def drain(ref, sem):
        pltpu.make_async_copy(ref, ref, sem).wait()

    small = []
    for i, (src, dst) in enumerate(((share_in, line), (norm_train, train), (norm_step, step))):
        small.append(pltpu.make_async_copy(src, dst, small_sem.at[i]))
        small[-1].start()

    early = pieces_of[len(cross_first)]
    (first_out,) = pieces_of[cross_first[-1]]
    late = [first_out] + [p for p in range(count) if p not in early + [first_out]]
    loading = early + late
    parts = {p: (early_part, k) for k, p in enumerate(early)}
    parts.update({p: (part, k) for k, p in enumerate(late)})

    def load(p):
        one, other, _, at = groups[p]
        for i, src in enumerate((one, other)):
            src = src.at[:, pl.ds(at, wide)]
            pltpu.make_async_copy(src, mixed.at[p, i], in_sem.at[p]).start()

    for p in loading[:WINDOW]:
        load(p)

    barrier = pltpu.get_barrier_semaphore()
    for d in range(1, n_rows):
        pl.semaphore_signal(
            barrier, inc=1, device_id={"rows": lax.rem(me + d, n_rows)}, device_id_type=MESH
        )

    envoy = me == 0
    row = n_width // 2
    along = [lane // row * row + (lane + d) % row for d in range(1, row)]
    opposite = (lane + row) % n_width

    @pl.when(envoy)
    def _():
        for peer in along + [opposite]:
            pl.semaphore_signal(barrier, inc=1, device_id={"width": peer}, device_id_type=MESH)

    for copy in small:
        copy.wait()
    piece_size = norm_train.shape[0]
    norm_at = pl.ds(len(late), 1)
    part[me, norm_at, :] = jnp.zeros((1, wide), jnp.float32)
    part[me, norm_at, pl.ds(0, piece_size)] = (train[...] + step[...]).reshape(1, -1)
    for at in range(0, depth, LANES):
        size = min(LANES, depth - at)
        piece = line[pl.ds(at, size)].reshape(1, size)
        share[pl.ds(at, size), :] = jnp.broadcast_to(piece, (LANES, size)).T

    core = me % 2
    place = (me // 2) % CIRCLE
    side = me // (2 * CIRCLE)

    def device(sides, steps, cores=0):
        chip = (side + sides) % 2 * CIRCLE + (place + steps + CIRCLE) % CIRCLE
        return chip * 2 + (core + cores) % 2

    far = [(a, b, c) for b in (2, 1, -1, 0) for a in (1, 0) for c in (1, 0) if (a, b, c) != (0, 0, 0)]

    def sum_up(p):
        drain(mixed.at[p], in_sem.at[p])
        if loading.index(p) + WINDOW < count:
            load(loading[loading.index(p) + WINDOW])

        def mix(i, acc):
            rows = pl.ds(pl.multiple_of(i * tile, tile), tile)
            s = share[rows, :]
            s = jnp.concatenate([s] * (wide // LANES), axis=1)
            r = s * mixed[p, 0, rows, :] + (1.0 - s) * mixed[p, 1, rows, :]
            mixed[p, 0, rows, :] = r
            return acc + jnp.sum((r * r).reshape(tile // 8, 8, wide), axis=0)

        acc = lax.fori_loop(0, depth // tile, mix, jnp.zeros((8, wide), jnp.float32))
        into, at_row = parts[p]
        into[me, pl.ds(at_row, 1), :] = jnp.sum(acc, axis=0, keepdims=True)

    def to_group(ref, sems):
        for where in far:
            pltpu.make_async_remote_copy(
                src_ref=ref.at[me],
                dst_ref=ref.at[me],
                send_sem=sems.at[0],
                recv_sem=sems.at[1],
                device_id={"rows": device(*where)},
                device_id_type=MESH,
            ).start()

    for p in early:
        sum_up(p)
    pl.semaphore_wait(barrier, n_rows - 1 + jnp.where(envoy, row, 0))
    to_group(early_part, early_sem)
    twin = me + 1 - 2 * core
    target = {UP: device(0, 1), DOWN: device(0, -1), ACROSS: device(1, 0)}
    sum_up(first_out)
    gone = stage.shape[1]
    for item in ahead:
        pltpu.make_async_remote_copy(
            src_ref=mixed.at[first_out, 0, pl.ds(0, gone), :],
            dst_ref=stage.at[item[0]],
            send_sem=stage_sem.at[0, item[0]],
            recv_sem=stage_sem.at[1, item[0]],
            device_id={"rows": target[item[0]]},
            device_id_type=MESH,
        ).start()
    for p in late[1:]:
        sum_up(p)
    to_group(part, sum_sem)

    slots = {}
    for event, _ in schedule:
        if not isinstance(event, int):
            slots[event] = len(slots)

    def size_of(item):
        return depth - gone if item in ahead else depth if is_whole(item) else half

    def whole(owner):
        return pl.ds(pl.multiple_of(owner * depth, half), depth)

    def part_of(owner, way):
        return pl.ds(pl.multiple_of(owner * depth + way * half, half), half)

    def held(item, sender):
        link, far, hop, _ = item
        if link == ACROSS:
            side_of = 0 if sender else 1
            owner = device(side_of, (0, -1, 1, 2, 2)[hop])
            return owner, None if hop < 3 else hop - 3
        away = hop - 1 if sender else hop
        return device(far, -away if link == UP else away), None if hop == 1 else link

    def rows_of(item, sender):
        owner, way = held(item, sender)
        if item in ahead:
            return pl.ds(pl.multiple_of(owner * depth + gone, 32), depth - gone)
        return whole(owner) if way is None else part_of(owner, way)

    def remote(item, sender):
        link, _, _, g = item
        ref = blocks[g].at[rows_of(item, sender), :]
        return pltpu.make_async_remote_copy(
            src_ref=ref,
            dst_ref=ref,
            send_sem=send_sem.at[link],
            recv_sem=recv_sem.at[slots[item]],
            device_id={"rows": target[link]},
            device_id_type=MESH,
        )

    sent = {}

    def send(item):
        remote(item, True).start()
        sent[item[0]] = sent.get(item[0], 0) + size_of(item) * len(pieces_of[item[3]])

    def share_with_twin(g, rows):
        ref = blocks[g].at[rows, :]
        pltpu.make_async_remote_copy(
            src_ref=ref,
            dst_ref=ref,
            send_sem=twin_sem.at[0, g // 2],
            recv_sem=twin_sem.at[1, g // 2],
            device_id={"rows": twin},
            device_id_type=MESH,
        ).start()

    def scales(ref, sems, size):
        drain(ref.at[pl.ds(0, n_rows - 1)], sems.at[1])
        total = ref[0, pl.ds(0, size), :]
        for d in range(1, n_rows):
            total = total + ref[d, pl.ds(0, size), :]
        scale = jnp.sqrt(total)
        return scale, 1.0 / scale

    early_scales = scales(early_part, early_sem, len(early))
    late_scales = None

    def take_in(item):
        link, _, _, g = item
        drain(stage.at[link], stage_sem.at[1, link])
        start = held(item, False)[0] * depth
        by = late_scales[1][:1, :]

        def narrow(i, carry):
            rows = pl.ds(pl.multiple_of(i * step_rows, step_rows), step_rows)
            here = pl.ds(pl.multiple_of(start + i * step_rows, step_rows), step_rows)
            blocks[g][here, :] = (stage[link, rows, :] * by).astype(blocks[g].dtype)
            return carry

        lax.fori_loop(0, gone // step_rows, narrow, 0)

    def make_block(g):
        pieces, out = pieces_of[g], blocks[g]
        scale, inverse = early_scales if pieces[0] in early else late_scales
        for p in pieces:
            _, _, col, at = groups[p]
            at_row = parts[p][1]
            col[pl.ds(at, wide)] = scale[at_row : at_row + 1, :].reshape(wide)

        def narrow(i, carry):
            rows = pl.ds(pl.multiple_of(i * tile, tile), tile)
            here = pl.ds(pl.multiple_of(me * depth + i * tile, tile), tile)
            for j, p in enumerate(pieces):
                at_row = parts[p][1]
                made = mixed[p, 0, rows, :] * inverse[at_row : at_row + 1, :]
                out[here, pl.ds(j * wide, wide)] = made.astype(out.dtype)
            return carry

        lax.fori_loop(0, depth // tile, narrow, 0)

    rows_half = n_rows // 2

    def meet():
        for d in range(n_rows):
            slab[lane, pl.ds(d % 2 * rows_half + d // 2, 1), :] = part[d, norm_at, :]
        for peer in along:
            pltpu.make_async_remote_copy(
                src_ref=slab.at[lane],
                dst_ref=slab.at[lane],
                send_sem=slab_sem.at[0, 0],
                recv_sem=slab_sem.at[0, 1],
                device_id={"width": peer},
                device_id_type=MESH,
            ).start()

    def swap():
        drain(slab.at[pl.ds(0, row - 1)], slab_sem.at[0, 1])
        mine = slab.at[pl.ds(lane // row * row, row)]
        pltpu.make_async_remote_copy(
            src_ref=mine,
            dst_ref=mine,
            send_sem=slab_sem.at[1, 0],
            recv_sem=slab_sem.at[1, 1],
            device_id={"width": opposite},
            device_id_type=MESH,
        ).start()

    def relay(way):
        return pltpu.make_async_remote_copy(
            src_ref=serve,
            dst_ref=serve,
            send_sem=relay_send.at[way],
            recv_sem=relay_recv.at[0],
            device_id={"rows": target.get(way, twin)},
            device_id_type=MESH,
        )

    def assemble():
        drain(slab.at[pl.ds(0, row)], slab_sem.at[1, 1])
        per_line = 2 * n_width * piece_size
        at_lane = lax.broadcasted_iota(jnp.int32, (rows_half, LANES), 1)
        tiles = [jnp.zeros((rows_half, LANES), jnp.float32)] * (per_line // LANES)
        for k in range(2 * n_width):
            x = slab[k % n_width, pl.ds(k // n_width * rows_half, rows_half), :]
            t, o = divmod(k * piece_size, LANES)
            x = pltpu.roll(x, o, 1) if o else x
            end = o + piece_size
            tiles[t] = jnp.where((at_lane >= o) & (at_lane < end), x, tiles[t])
            if end > LANES:
                tiles[t + 1] = jnp.where(at_lane < end - LANES, x, tiles[t + 1])
        for t, x in enumerate(tiles):
            for a in range(rows_half):
                flat[pl.ds(a * per_line + t * LANES, LANES)] = x[a : a + 1, :].reshape(LANES)
        serve[...] = flat[...].astype(serve.dtype)

    TWIN = 3
    lead = core == 0
    duties = [
        (envoy, (UP, DOWN, ACROSS, TWIN)),
        (lead & (place == 0) & (side == 1), (UP, DOWN, TWIN)),
        (lead & (place == 1), (UP, TWIN)),
        (lead & (place == 3), (TWIN,)),
        (lead & (place == 2), (TWIN,)),
        (core == 1, ()),
    ]

    def duty(i):
        role, ways = duties[i]

        @pl.when(role)
        def _():
            if i == 0:
                assemble()
            else:
                drain(serve, relay_recv.at[0])
            for way in ways:
                relay(way).start()

    moments = [len(schedule) * (3 + i) // 12 for i in range(len(duties))]
    meeting, swapping = len(blocks), (len(blocks) + moments[0]) // 2
    for index, (event, items) in enumerate(schedule):
        if index == meeting:
            pl.when(envoy)(meet)
        if index == swapping:
            pl.when(envoy)(swap)
        if index in moments:
            duty(moments.index(index))
        if isinstance(event, int):
            if late_scales is None and pieces_of[event][0] in late:
                late_scales = scales(part, sum_sem, len(late))
            make_block(event)
            g, rows = event, whole(me)
        else:
            if event in ahead:
                take_in(event)
            remote(event, False).wait_recv()
            g = event[3]
            rows = whole(held(event, False)[0]) if event in ahead else rows_of(event, False)
        for item in items:
            send(item)
        if not isinstance(event, int):
            share_with_twin(g, rows)
        if index == 2 * len(blocks):
            for b in range(len(blocks)):
                share_with_twin(b, whole(me))

    def drain_rows(rows, sem):
        drain(blocks[0].at[pl.ds(0, rows // len(pieces_of[0])), :], sem)

    for item in ahead:
        drain(stage.at[item[0]], stage_sem.at[0, item[0]])
    for link, rows in sent.items():
        drain_rows(rows, send_sem.at[link])
    for g in range(0, len(blocks), 2):
        for way in range(2):
            rows = depth * n_rows // 2 * sum(len(pieces) for pieces in pieces_of[g : g + 2])
            drain_rows(rows, twin_sem.at[way, g // 2])
    drain(early_part.at[pl.ds(0, n_rows - 1)], early_sem.at[0])
    drain(part.at[pl.ds(0, n_rows - 1)], sum_sem.at[0])
    for i, (role, ways) in enumerate(duties):

        @pl.when(role)
        def _(i=i, ways=ways):
            if i == 0:
                drain(slab.at[pl.ds(0, row - 1)], slab_sem.at[0, 0])
                drain(slab.at[pl.ds(0, row)], slab_sem.at[1, 0])
            for way in ways:
                relay(way).wait_send()


def store(pieces_of, wide, *refs):
    outs, sem = refs[-8:-1], refs[-1]
    blocks, small = refs[:-12], refs[-12:-8]
    pairs = list(zip(small, outs[3:]))
    for pieces, block in zip(pieces_of, blocks):
        lone = [p for p in pieces if p < 2]
        for j, p in enumerate(lone):
            pairs.append((block.at[:, pl.ds(j * wide, wide)], outs[1 + p]))
        if pieces[len(lone) :]:
            at, size = (pieces[len(lone)] - 2) * wide, (len(pieces) - len(lone)) * wide
            pairs.append((block.at[:, pl.ds(len(lone) * wide, size)], outs[0].at[:, pl.ds(at, size)]))
    copies = [pltpu.make_async_copy(src, dst, sem.at[i]) for i, (src, dst) in enumerate(pairs)]
    for copy in copies:
        copy.start()
    for copy in copies:
        copy.wait()


def solution(mesh):
    n_rows, n_width = mesh.shape["rows"], mesh.shape["width"]

    def shards(
        one_query,
        other_query,
        one_key,
        other_key,
        one_value,
        other_value,
        mix_share,
        norm_train,
        norm_step,
    ):
        depth, wide = one_key.shape
        wide_query = one_query.shape[1]
        count = 2 + wide_query // wide
        pieces_of, cross_first = layout(count)
        n_blocks = len(pieces_of)
        ahead = ahead_of(cross_first)
        gone = depth * 5 // 7 // 32 * 32
        schedule = plan([len(pieces) for pieces in pieces_of], cross_first, ahead, gone / depth)
        n_items = len(schedule) - n_blocks
        n_early = len(pieces_of[len(cross_first)])
        piece = norm_train.shape[0]
        total = depth * n_rows
        hbm = pl.BlockSpec(memory_space=pltpu.HBM)
        vmem = pl.BlockSpec(memory_space=pltpu.VMEM)
        dma = pltpu.SemaphoreType.DMA
        out_shape = tuple(
            pltpu.VMEM((total, wide * len(pieces)), jnp.bfloat16) for pieces in pieces_of
        ) + (
            pltpu.VMEM((wide_query,), jnp.float32),
            pltpu.VMEM((wide,), jnp.float32),
            pltpu.VMEM((wide,), jnp.float32),
            pltpu.VMEM((n_rows * n_width * piece,), jnp.bfloat16),
        )
        gathered = pl.pallas_call(
            lambda *refs: kernel(n_rows, n_width, pieces_of, cross_first, ahead, schedule, *refs),
            out_shape=out_shape,
            in_specs=[hbm] * 9,
            out_specs=[vmem] * (n_blocks + 4),
            scratch_shapes=[
                pltpu.VMEM((count, 2, depth, wide), jnp.float32),
                pltpu.VMEM((depth, LANES), jnp.float32),
                pltpu.VMEM((depth,), jnp.float32),
                pltpu.VMEM((piece,), jnp.float32),
                pltpu.VMEM((piece,), jnp.float32),
                pltpu.VMEM((n_rows, n_early, wide), jnp.float32),
                pltpu.VMEM((n_rows, count - n_early + 1, wide), jnp.float32),
                pltpu.VMEM((n_width, n_rows, LANES), jnp.float32),
                pltpu.VMEM((n_rows * n_width * piece,), jnp.float32),
                dma((count,)),
                dma((3,)),
                dma((2, 2)),
                dma((4,)),
                dma((1,)),
                dma((2,)),
                dma((2,)),
                dma((3,)),
                dma((n_items,)),
                dma((2, (n_blocks + 1) // 2)),
                pltpu.VMEM((3, gone, wide), jnp.float32),
                dma((2, 3)),
            ],
            compiler_params=pltpu.CompilerParams(
                collective_id=0, has_side_effects=True, vmem_limit_bytes=44 * 1024 * 1024
            ),
        )(mix_share, norm_train, norm_step, one_query, other_query, one_key, other_key, one_value, other_value)
        return pl.pallas_call(
            lambda *refs: store(pieces_of, wide, *refs),
            out_shape=(
                jax.ShapeDtypeStruct((total, wide_query), jnp.bfloat16),
                jax.ShapeDtypeStruct((total, wide), jnp.bfloat16),
                jax.ShapeDtypeStruct((total, wide), jnp.bfloat16),
            )
            + tuple(jax.ShapeDtypeStruct(o.shape, o.dtype) for o in out_shape[n_blocks:]),
            in_specs=[vmem] * (n_blocks + 4),
            out_specs=[hbm] * 7,
            scratch_shapes=[dma((count + 4,))],
            compiler_params=pltpu.CompilerParams(vmem_limit_bytes=1024 * 1024),
        )(*gathered)

    wide_spec = P("rows", "width")
    in_specs = (wide_spec,) * 6 + (P("rows"), P(("rows", "width")), P(("rows", "width")))
    out_specs = (P(None, "width"),) * 3 + (P("width"),) * 3 + (P(),)
    return jax.shard_map(shards, mesh=mesh, in_specs=in_specs, out_specs=out_specs, check_vma=False)
```

```python
import jax
import jax.numpy as jnp
from jax import lax
from jax.experimental import pallas as pl
from jax.experimental.pallas import tpu as pltpu
from jax.sharding import PartitionSpec as P

MESH = pl.DeviceIdType.MESH
LANES = 128
CIRCLE = 4
UP, DOWN, ACROSS = 0, 1, 2
SPAN = 2
WINDOW = 4
DEPTH = 9
LAG = 0.7


def layout(count):
    first = (5 * count + 4) // 9

    def cut(start, end):
        return [list(range(i, min(i + SPAN, end))) for i in range(start, end, SPAN)]

    blocks = cut(0, first) + cut(first, count)
    return blocks, [b for b, pieces in enumerate(blocks) if pieces[0] < first]


def ahead_of(cross_first):
    last = cross_first[-1]
    return (UP, 0, 1, last), (DOWN, 0, 1, last), (ACROSS, 0, 0, last)


def plan(weights, cross_first, ahead, gone):
    free, flying, ready = [0.0] * 3, [0] * 3, [[], [], []]
    events, order, clock = [], [], [0]

    def put(now, event):
        clock[0] += 1
        events.append((now, clock[0], event))

    def offer(item):
        clock[0] += 1
        ready[item[0]].append((-steps_after(item, cross_first), clock[0], item))

    first = cross_first
    second = [b for b in range(len(weights)) if b not in cross_first]
    for b in (3, 0, 1, 4, 2):
        put(0.1 * len(events), b)
    while events:
        events.sort()
        now, _, event = events.pop(0)
        if isinstance(event, int):
            for item in ((ACROSS, 0, 0, event), (UP, 0, 1, event), (DOWN, 0, 1, event)):
                offer(item)
        else:
            flying[event[0]] -= 1
            for item in followers(event, cross_first):
                offer(item)
        sends = []
        for link in (ACROSS, UP, DOWN):
            ready[link].sort()
            while ready[link] and flying[link] < DEPTH:
                item = ready[link].pop(0)[2]
                flying[link] += 1
                size = 1.0 - gone if item in ahead else 1.0 if is_whole(item) else 0.5
                free[link] = max(free[link], now) + size * weights[item[3]]
                put(free[link] + LAG, item)
                sends.append(item)
        order.append((event, sends))
    return order


def steps_after(item, cross_first):
    return max([1 + steps_after(x, cross_first) for x in followers(item, cross_first)], default=0)


def is_whole(item):
    link, _, hop, _ = item
    return hop < 3 if link == ACROSS else hop == 1


def followers(item, cross_first):
    link, far, hop, g = item
    if link == ACROSS:
        return [(UP, 1, 1, g), (DOWN, 1, 1, g)] if g in cross_first else []
    steps = [(link, far, 2, g)] if hop == 1 else []
    if g not in cross_first:
        steps.append((ACROSS, 0, 1 + link if hop == 1 else 3 + link, g))
    return steps


def kernel(
    n_rows,
    n_width,
    pieces_of,
    cross_first,
    ahead,
    schedule,
    share_in,
    norm_train,
    norm_step,
    one_query,
    other_query,
    one_key,
    other_key,
    one_value,
    other_value,
    *refs,
):
    blocks = refs[: len(pieces_of)]
    col_query, col_key, col_value, serve, mixed, share = refs[len(blocks) :][:6]
    line, train, step, early_part, part, slab, flat = refs[len(blocks) + 6 :][:7]
    in_sem, small_sem, slab_sem, relay_send, relay_recv = refs[len(blocks) + 13 :][:5]
    early_sem, sum_sem, send_sem, recv_sem, twin_sem = refs[len(blocks) + 18 :][:5]
    stage, stage_sem = refs[len(blocks) + 23 :]
    me = lax.axis_index("rows")
    lane = lax.axis_index("width")
    depth, wide = one_key.shape
    groups = [
        (one_key, other_key, col_key, 0),
        (one_value, other_value, col_value, 0),
    ] + [
        (one_query, other_query, col_query, j * wide)
        for j in range(one_query.shape[1] // wide)
    ]
    count = len(groups)
    tile = 64 if depth % 64 == 0 else 16
    half = depth // 2
    step_rows = 32

    def drain(ref, sem):
        pltpu.make_async_copy(ref, ref, sem).wait()

    small = []
    for i, (src, dst) in enumerate(((share_in, line), (norm_train, train), (norm_step, step))):
        small.append(pltpu.make_async_copy(src, dst, small_sem.at[i]))
        small[-1].start()

    early = pieces_of[3]
    (first_out,) = pieces_of[cross_first[-1]]
    late = [first_out] + [p for p in range(count) if p not in early + [first_out]]
    loading = early + late
    parts = {p: (early_part, k) for k, p in enumerate(early)}
    parts.update({p: (part, k) for k, p in enumerate(late)})

    def load(p):
        one, other, _, at = groups[p]
        for i, src in enumerate((one, other)):
            src = src.at[:, pl.ds(at, wide)]
            pltpu.make_async_copy(src, mixed.at[p, i], in_sem.at[p]).start()

    for p in loading[:WINDOW]:
        load(p)

    barrier = pltpu.get_barrier_semaphore()
    for d in range(1, n_rows):
        pl.semaphore_signal(
            barrier, inc=1, device_id={"rows": lax.rem(me + d, n_rows)}, device_id_type=MESH
        )

    envoy = me == 0
    row = n_width // 2
    along = [lane // row * row + (lane + d) % row for d in range(1, row)]
    opposite = (lane + row) % n_width

    @pl.when(envoy)
    def _():
        for peer in along + [opposite]:
            pl.semaphore_signal(barrier, inc=1, device_id={"width": peer}, device_id_type=MESH)

    for copy in small:
        copy.wait()
    piece_size = norm_train.shape[0]
    norm_at = pl.ds(len(late), 1)
    part[me, norm_at, :] = jnp.zeros((1, wide), jnp.float32)
    part[me, norm_at, pl.ds(0, piece_size)] = (train[...] + step[...]).reshape(1, -1)
    for at in range(0, depth, LANES):
        size = min(LANES, depth - at)
        piece = line[pl.ds(at, size)].reshape(1, size)
        share[pl.ds(at, size), :] = jnp.broadcast_to(piece, (LANES, size)).T

    core = me % 2
    place = (me // 2) % CIRCLE
    side = me // (2 * CIRCLE)

    def device(sides, steps, cores=0):
        chip = (side + sides) % 2 * CIRCLE + (place + steps + CIRCLE) % CIRCLE
        return chip * 2 + (core + cores) % 2

    far = [(a, b, c) for b in (2, 1, -1, 0) for a in (1, 0) for c in (1, 0) if (a, b, c) != (0, 0, 0)]

    def sum_up(p):
        drain(mixed.at[p], in_sem.at[p])
        if loading.index(p) + WINDOW < count:
            load(loading[loading.index(p) + WINDOW])

        def mix(i, acc):
            rows = pl.ds(pl.multiple_of(i * tile, tile), tile)
            s = share[rows, :]
            s = jnp.concatenate([s] * (wide // LANES), axis=1)
            r = s * mixed[p, 0, rows, :] + (1.0 - s) * mixed[p, 1, rows, :]
            mixed[p, 0, rows, :] = r
            return acc + jnp.sum((r * r).reshape(tile // 8, 8, wide), axis=0)

        acc = lax.fori_loop(0, depth // tile, mix, jnp.zeros((8, wide), jnp.float32))
        into, at_row = parts[p]
        into[me, pl.ds(at_row, 1), :] = jnp.sum(acc, axis=0, keepdims=True)

    def to_group(ref, sems):
        for where in far:
            pltpu.make_async_remote_copy(
                src_ref=ref.at[me],
                dst_ref=ref.at[me],
                send_sem=sems.at[0],
                recv_sem=sems.at[1],
                device_id={"rows": device(*where)},
                device_id_type=MESH,
            ).start()

    for p in early:
        sum_up(p)
    pl.semaphore_wait(barrier, n_rows - 1 + jnp.where(envoy, row, 0))
    to_group(early_part, early_sem)
    twin = me + 1 - 2 * core
    target = {UP: device(0, 1), DOWN: device(0, -1), ACROSS: device(1, 0)}
    sum_up(first_out)
    gone = stage.shape[1]
    for item in ahead:
        pltpu.make_async_remote_copy(
            src_ref=mixed.at[first_out, 0, pl.ds(0, gone), :],
            dst_ref=stage.at[item[0]],
            send_sem=stage_sem.at[0, item[0]],
            recv_sem=stage_sem.at[1, item[0]],
            device_id={"rows": target[item[0]]},
            device_id_type=MESH,
        ).start()
    for p in late[1:]:
        sum_up(p)
    to_group(part, sum_sem)

    slots = {}
    for event, _ in schedule:
        if not isinstance(event, int):
            slots[event] = len(slots)

    def size_of(item):
        return depth - gone if item in ahead else depth if is_whole(item) else half

    def whole(owner):
        return pl.ds(pl.multiple_of(owner * depth, half), depth)

    def part_of(owner, way):
        return pl.ds(pl.multiple_of(owner * depth + way * half, half), half)

    def held(item, sender):
        link, far, hop, _ = item
        if link == ACROSS:
            side_of = 0 if sender else 1
            owner = device(side_of, (0, -1, 1, 2, 2)[hop])
            return owner, None if hop < 3 else hop - 3
        away = hop - 1 if sender else hop
        return device(far, -away if link == UP else away), None if hop == 1 else link

    def rows_of(item, sender):
        owner, way = held(item, sender)
        if item in ahead:
            return pl.ds(pl.multiple_of(owner * depth + gone, 32), depth - gone)
        return whole(owner) if way is None else part_of(owner, way)

    def remote(item, sender):
        link, _, _, g = item
        ref = blocks[g].at[rows_of(item, sender), :]
        return pltpu.make_async_remote_copy(
            src_ref=ref,
            dst_ref=ref,
            send_sem=send_sem.at[link],
            recv_sem=recv_sem.at[slots[item]],
            device_id={"rows": target[link]},
            device_id_type=MESH,
        )

    sent = {}

    def send(item):
        remote(item, True).start()
        sent[item[0]] = sent.get(item[0], 0) + size_of(item) * len(pieces_of[item[3]])

    def share_with_twin(g, rows):
        ref = blocks[g].at[rows, :]
        pltpu.make_async_remote_copy(
            src_ref=ref,
            dst_ref=ref,
            send_sem=twin_sem.at[0, g // 2],
            recv_sem=twin_sem.at[1, g // 2],
            device_id={"rows": twin},
            device_id_type=MESH,
        ).start()

    def scales(ref, sems, size):
        drain(ref.at[pl.ds(0, n_rows - 1)], sems.at[1])
        total = ref[0, pl.ds(0, size), :]
        for d in range(1, n_rows):
            total = total + ref[d, pl.ds(0, size), :]
        scale = jnp.sqrt(total)
        return scale, 1.0 / scale

    early_scales = scales(early_part, early_sem, len(early))
    late_scales = None

    def take_in(item):
        link, _, _, g = item
        drain(stage.at[link], stage_sem.at[1, link])
        start = held(item, False)[0] * depth
        by = late_scales[1][:1, :]

        def narrow(i, carry):
            rows = pl.ds(pl.multiple_of(i * step_rows, step_rows), step_rows)
            here = pl.ds(pl.multiple_of(start + i * step_rows, step_rows), step_rows)
            blocks[g][here, :] = (stage[link, rows, :] * by).astype(blocks[g].dtype)
            return carry

        lax.fori_loop(0, gone // step_rows, narrow, 0)

    def make_block(g):
        pieces, out = pieces_of[g], blocks[g]
        scale, inverse = early_scales if pieces[0] in early else late_scales
        for p in pieces:
            _, _, col, at = groups[p]
            at_row = parts[p][1]
            col[pl.ds(at, wide)] = scale[at_row : at_row + 1, :].reshape(wide)

        def narrow(i, carry):
            rows = pl.ds(pl.multiple_of(i * tile, tile), tile)
            here = pl.ds(pl.multiple_of(me * depth + i * tile, tile), tile)
            for j, p in enumerate(pieces):
                at_row = parts[p][1]
                made = mixed[p, 0, rows, :] * inverse[at_row : at_row + 1, :]
                out[here, pl.ds(j * wide, wide)] = made.astype(out.dtype)
            return carry

        lax.fori_loop(0, depth // tile, narrow, 0)

    rows_half = n_rows // 2

    def meet():
        for d in range(n_rows):
            slab[lane, pl.ds(d % 2 * rows_half + d // 2, 1), :] = part[d, norm_at, :]
        for peer in along:
            pltpu.make_async_remote_copy(
                src_ref=slab.at[lane],
                dst_ref=slab.at[lane],
                send_sem=slab_sem.at[0, 0],
                recv_sem=slab_sem.at[0, 1],
                device_id={"width": peer},
                device_id_type=MESH,
            ).start()

    def swap():
        drain(slab.at[pl.ds(0, row - 1)], slab_sem.at[0, 1])
        mine = slab.at[pl.ds(lane // row * row, row)]
        pltpu.make_async_remote_copy(
            src_ref=mine,
            dst_ref=mine,
            send_sem=slab_sem.at[1, 0],
            recv_sem=slab_sem.at[1, 1],
            device_id={"width": opposite},
            device_id_type=MESH,
        ).start()

    def relay(way):
        return pltpu.make_async_remote_copy(
            src_ref=serve,
            dst_ref=serve,
            send_sem=relay_send.at[way],
            recv_sem=relay_recv.at[0],
            device_id={"rows": target.get(way, twin)},
            device_id_type=MESH,
        )

    def assemble():
        drain(slab.at[pl.ds(0, row)], slab_sem.at[1, 1])
        per_line = 2 * n_width * piece_size
        at_lane = lax.broadcasted_iota(jnp.int32, (rows_half, LANES), 1)
        tiles = [jnp.zeros((rows_half, LANES), jnp.float32)] * (per_line // LANES)
        for k in range(2 * n_width):
            x = slab[k % n_width, pl.ds(k // n_width * rows_half, rows_half), :]
            t, o = divmod(k * piece_size, LANES)
            x = pltpu.roll(x, o, 1) if o else x
            end = o + piece_size
            tiles[t] = jnp.where((at_lane >= o) & (at_lane < end), x, tiles[t])
            if end > LANES:
                tiles[t + 1] = jnp.where(at_lane < end - LANES, x, tiles[t + 1])
        for t, x in enumerate(tiles):
            for a in range(rows_half):
                flat[pl.ds(a * per_line + t * LANES, LANES)] = x[a : a + 1, :].reshape(LANES)
        serve[...] = flat[...].astype(serve.dtype)

    TWIN = 3
    lead = core == 0
    duties = [
        (envoy, (UP, DOWN, ACROSS, TWIN)),
        (lead & (place == 0) & (side == 1), (UP, DOWN, TWIN)),
        (lead & (place == 1), (UP, TWIN)),
        (lead & (place == 3), (TWIN,)),
        (lead & (place == 2), (TWIN,)),
        (core == 1, ()),
    ]

    def duty(i):
        role, ways = duties[i]

        @pl.when(role)
        def _():
            if i == 0:
                assemble()
            else:
                drain(serve, relay_recv.at[0])
            for way in ways:
                relay(way).start()

    moments = [len(schedule) * (3 + i) // 12 for i in range(len(duties))]
    meeting, swapping = len(blocks), (len(blocks) + moments[0]) // 2
    for index, (event, items) in enumerate(schedule):
        if index == meeting:
            pl.when(envoy)(meet)
        if index == swapping:
            pl.when(envoy)(swap)
        if index in moments:
            duty(moments.index(index))
        if isinstance(event, int):
            if late_scales is None and pieces_of[event][0] in late:
                late_scales = scales(part, sum_sem, len(late))
            make_block(event)
            g, rows = event, whole(me)
        else:
            if event in ahead:
                take_in(event)
            remote(event, False).wait_recv()
            g = event[3]
            rows = whole(held(event, False)[0]) if event in ahead else rows_of(event, False)
        for item in items:
            send(item)
        share_with_twin(g, rows)

    def drain_rows(rows, sem):
        drain(blocks[0].at[pl.ds(0, rows // len(pieces_of[0])), :], sem)

    for item in ahead:
        drain(stage.at[item[0]], stage_sem.at[0, item[0]])
    for link, rows in sent.items():
        drain_rows(rows, send_sem.at[link])
    for g in range(0, len(blocks), 2):
        for way in range(2):
            rows = depth * n_rows // 2 * sum(len(pieces) for pieces in pieces_of[g : g + 2])
            drain_rows(rows, twin_sem.at[way, g // 2])
    drain(early_part.at[pl.ds(0, n_rows - 1)], early_sem.at[0])
    drain(part.at[pl.ds(0, n_rows - 1)], sum_sem.at[0])
    for i, (role, ways) in enumerate(duties):

        @pl.when(role)
        def _(i=i, ways=ways):
            if i == 0:
                drain(slab.at[pl.ds(0, row - 1)], slab_sem.at[0, 0])
                drain(slab.at[pl.ds(0, row)], slab_sem.at[1, 0])
            for way in ways:
                relay(way).wait_send()


def store(pieces_of, wide, *refs):
    outs, sem = refs[-8:-1], refs[-1]
    blocks, small = refs[:-12], refs[-12:-8]
    pairs = list(zip(small, outs[3:]))
    for pieces, block in zip(pieces_of, blocks):
        lone = [p for p in pieces if p < 2]
        for j, p in enumerate(lone):
            pairs.append((block.at[:, pl.ds(j * wide, wide)], outs[1 + p]))
        if pieces[len(lone) :]:
            at, size = (pieces[len(lone)] - 2) * wide, (len(pieces) - len(lone)) * wide
            pairs.append((block.at[:, pl.ds(len(lone) * wide, size)], outs[0].at[:, pl.ds(at, size)]))
    copies = [pltpu.make_async_copy(src, dst, sem.at[i]) for i, (src, dst) in enumerate(pairs)]
    for copy in copies:
        copy.start()
    for copy in copies:
        copy.wait()


def solution(mesh):
    n_rows, n_width = mesh.shape["rows"], mesh.shape["width"]

    def shards(
        one_query,
        other_query,
        one_key,
        other_key,
        one_value,
        other_value,
        mix_share,
        norm_train,
        norm_step,
    ):
        depth, wide = one_key.shape
        wide_query = one_query.shape[1]
        count = 2 + wide_query // wide
        pieces_of, cross_first = layout(count)
        n_blocks = len(pieces_of)
        ahead = ahead_of(cross_first)
        gone = depth * 5 // 7 // 32 * 32
        schedule = plan([len(pieces) for pieces in pieces_of], cross_first, ahead, gone / depth)
        n_items = len(schedule) - n_blocks
        n_early = len(pieces_of[3])
        piece = norm_train.shape[0]
        total = depth * n_rows
        hbm = pl.BlockSpec(memory_space=pltpu.HBM)
        vmem = pl.BlockSpec(memory_space=pltpu.VMEM)
        dma = pltpu.SemaphoreType.DMA
        out_shape = tuple(
            pltpu.VMEM((total, wide * len(pieces)), jnp.bfloat16) for pieces in pieces_of
        ) + (
            pltpu.VMEM((wide_query,), jnp.float32),
            pltpu.VMEM((wide,), jnp.float32),
            pltpu.VMEM((wide,), jnp.float32),
            pltpu.VMEM((n_rows * n_width * piece,), jnp.bfloat16),
        )
        gathered = pl.pallas_call(
            lambda *refs: kernel(n_rows, n_width, pieces_of, cross_first, ahead, schedule, *refs),
            out_shape=out_shape,
            in_specs=[hbm] * 9,
            out_specs=[vmem] * (n_blocks + 4),
            scratch_shapes=[
                pltpu.VMEM((count, 2, depth, wide), jnp.float32),
                pltpu.VMEM((depth, LANES), jnp.float32),
                pltpu.VMEM((depth,), jnp.float32),
                pltpu.VMEM((piece,), jnp.float32),
                pltpu.VMEM((piece,), jnp.float32),
                pltpu.VMEM((n_rows, n_early, wide), jnp.float32),
                pltpu.VMEM((n_rows, count - n_early + 1, wide), jnp.float32),
                pltpu.VMEM((n_width, n_rows, LANES), jnp.float32),
                pltpu.VMEM((n_rows * n_width * piece,), jnp.float32),
                dma((count,)),
                dma((3,)),
                dma((2, 2)),
                dma((4,)),
                dma((1,)),
                dma((2,)),
                dma((2,)),
                dma((3,)),
                dma((n_items,)),
                dma((2, (n_blocks + 1) // 2)),
                pltpu.VMEM((3, gone, wide), jnp.float32),
                dma((2, 3)),
            ],
            compiler_params=pltpu.CompilerParams(
                collective_id=0, has_side_effects=True, vmem_limit_bytes=44 * 1024 * 1024
            ),
        )(mix_share, norm_train, norm_step, one_query, other_query, one_key, other_key, one_value, other_value)
        return pl.pallas_call(
            lambda *refs: store(pieces_of, wide, *refs),
            out_shape=(
                jax.ShapeDtypeStruct((total, wide_query), jnp.bfloat16),
                jax.ShapeDtypeStruct((total, wide), jnp.bfloat16),
                jax.ShapeDtypeStruct((total, wide), jnp.bfloat16),
            )
            + tuple(jax.ShapeDtypeStruct(o.shape, o.dtype) for o in out_shape[n_blocks:]),
            in_specs=[vmem] * (n_blocks + 4),
            out_specs=[hbm] * 7,
            scratch_shapes=[dma((n_blocks + 5,))],
            compiler_params=pltpu.CompilerParams(vmem_limit_bytes=1024 * 1024),
        )(*gathered)

    wide_spec = P("rows", "width")
    in_specs = (wide_spec,) * 6 + (P("rows"), P(("rows", "width")), P(("rows", "width")))
    out_specs = (P(None, "width"),) * 3 + (P("width"),) * 3 + (P(),)
    return jax.shard_map(shards, mesh=mesh, in_specs=in_specs, out_specs=out_specs, check_vma=False)
```
